128 devices in a mesh: mem: 8 (over z_lo, y), sx: 4 (over z_hi, core), sy: 4 (over x).
Axes of the slice: x: 4, y: 4, z: 4 (z_hi: 2, z_lo: 2; z = z_hi * 2 + z_lo), core: 2. Of those that a mesh axis runs over, the one named last changes fastest.
Arguments:
- child: bfloat16 [32, 8, 192, 3072], P('mem', None, 'sx', 'sy'), may hold values from -13 to 13
Outputs:
- parent_mean: float32 [8, 64, 1024], P('mem', 'sx', 'sy')
- local_cov: float32 [64, 64, 1024], P('mem', 'sx', 'sy')
The draws below stay inside these ranges and needn't reach their ends.
All inputs are finite; a program needn't handle non-finite values.
Results may differ from the reference program's by a relative error of at most 0.002.
Values sent between devices are 32-bit elements; how exact they have to be, the bound alone decides.
A program may use at most 192 MiB of HBM per device.

```python
import jax
import jax.numpy as jnp
import numpy as np
from jax import lax

L = 8
HALO = 4
M = 32
NX = 64
NY = 1024


def draw_child(key, part):
    base_key = jax.random.fold_in(key, 11)
    noise_key = jax.random.fold_in(key, 12)
    rows = 3 * NX
    cols = 3 * NY
    xpos = jnp.arange(rows, dtype=jnp.float32) / max(rows - 1, 1)
    xscale = (1.0 + 2.0 * xpos)[None, None, :, None]
    base = jax.random.uniform(base_key, (1, L, rows, cols), jnp.float32, -1.0, 1.0)
    noise = jax.random.truncated_normal(noise_key, -4.0, 4.0, (M, L, rows, cols), jnp.float32)
    values = base + xscale * noise
    return values.astype(jnp.bfloat16)


def setup_inputs(seed: int = 0) -> dict:
    splits = jax.random.split(jax.random.key(seed), 2)
    return {
        "child": draw_child(jax.random.fold_in(splits[1], 71), 0),
    }


def gaspari_table(reach):
    offsets = np.arange(-reach, reach + 1) * 1.0
    dist = np.sqrt(offsets[:, None] ** 2 + offsets[None, :] ** 2) / 2.5
    near = -0.25 * dist ** 5 + 0.5 * dist ** 4 + 0.625 * dist ** 3 - 5.0 / 3.0 * dist ** 2 + 1.0
    safe = np.maximum(dist, 0.001)
    far = dist ** 5 / 12.0 - 0.5 * dist ** 4 + 0.625 * dist ** 3 + 5.0 / 3.0 * dist ** 2 - 5.0 * dist + 4.0 - 2.0 / (3.0 * safe)
    table = np.where(dist <= 1.0, near, np.where(dist < 2.0, far, 0.0))
    return table / table.sum()

def reference(child):
    parent = lax.optimization_barrier(jnp.sum(child.reshape(M, L, NX, 3, NY, 3), axis=(3, 5), dtype=jnp.float32)) / 9.0
    parent_mean = lax.optimization_barrier(jnp.sum(parent, axis=0)) / M
    anomaly = parent - parent_mean[None]
    cov = jnp.einsum('alxy,akxy->lkxy', anomaly, anomaly) / (M - 1)
    cov = cov.reshape(L * L, NX, NY)
    diag = jnp.stack([cov[l * L + l] for l in range(L)])
    spread = jnp.sum(diag) / (L * NX * NY)
    table = gaspari_table(HALO)
    padded = jnp.pad(cov, ((0, 0), (HALO, HALO), (HALO, HALO)))
    smoothed = jnp.zeros((L * L, NX, NY), jnp.float32)
    for a in range(2 * HALO + 1):
        for b in range(2 * HALO + 1):
            weight = float(table[a, b])
            if weight != 0.0:
                smoothed = smoothed + weight * padded[:, a:a + NX, b:b + NY]
    return (parent_mean, smoothed / (spread + 1e-06))
```

```python
import functools

import jax
import jax.numpy as jnp
import numpy as np
from jax import lax
from jax.experimental import pallas as pl
from jax.experimental.pallas import tpu as pltpu
from jax.sharding import PartitionSpec as P

MESH = pl.DeviceIdType.MESH
REACH = 4
LANES = 128
SUB = 8


def gaspari_table(reach):
    offsets = np.arange(-reach, reach + 1) * 1.0
    dist = np.sqrt(offsets[:, None] ** 2 + offsets[None, :] ** 2) / 2.5
    near = -0.25 * dist**5 + 0.5 * dist**4 + 0.625 * dist**3 - 5.0 / 3.0 * dist**2 + 1.0
    safe = np.maximum(dist, 0.001)
    far = (
        dist**5 / 12.0
        - 0.5 * dist**4
        + 0.625 * dist**3
        + 5.0 / 3.0 * dist**2
        - 5.0 * dist
        + 4.0
        - 2.0 / (3.0 * safe)
    )
    table = np.where(dist <= 1.0, near, np.where(dist < 2.0, far, 0.0))
    return table / table.sum()


def kernel(
    nmem,
    nsx,
    nsy,
    child_ref,
    mean_ref,
    cov_ref,
    xbuf,
    ybuf,
    psend,
    rbuf,
    abuf,
    mbuf,
    msg,
    q,
    edge_l,
    edge_r,
    hsend,
    h,
    zbuf,
    s1,
    s2,
    ld_sem,
    p1_send,
    p1_recv,
    s1_send,
    s1_recv,
    e_send,
    e_recv,
    q_send,
    q_recv,
    r_send,
    h_send,
    h_recv,
    g_send,
    s2_send,
    s2_recv,
):
    members, levels, child_rows, child_cols = child_ref.shape
    rows = child_rows // 3
    mem = lax.axis_index("mem")
    sx = lax.axis_index("sx")
    sy = lax.axis_index("sy")
    total_members = members * nmem

    def at(m, x, y):
        return {"mem": m, "sx": x, "sy": y}

    loads = []
    for m in range(members):
        copy = pltpu.make_async_copy(child_ref.at[m], xbuf.at[m], ld_sem.at[m])
        copy.start()
        loads.append(copy)

    barrier = pltpu.get_barrier_semaphore()
    greeted = 0

    def greet(m, x, y):
        pl.semaphore_signal(barrier, inc=1, device_id=at(m, x, y), device_id_type=MESH)

    mem_peers = [lax.rem(mem + o, nmem) for o in range(nmem)]
    plane = [(a, b) for a in range(nsx) for b in range(nsy) if (a, b) != (0, 0)]
    plane_peers = [(lax.rem(sx + a, nsx), lax.rem(sy + b, nsy)) for a, b in plane]
    for o in range(1, nmem):
        greet(mem_peers[o], sx, sy)
        greeted += 1
    for x, y in plane_peers:
        greet(mem, x, y)
        greeted += 1
    for a in (1, nsx - 1):
        for o in range(1, nmem):
            greet(mem_peers[o], lax.rem(sx + a, nsx), sy)
            greeted += 1

    zero = jnp.zeros((SUB, LANES), jnp.float32)

    @pl.when(sx == 0)
    def _():
        for s in range(2):
            for v in range(5):
                q[s, v] = zero
            for v in range(2):
                h[s, v] = zero

    @pl.when(sx == nsx - 1)
    def _():
        for s in range(nmem + 2, nmem + 4):
            for v in range(5):
                q[s, v] = zero
            for v in range(2):
                h[s, v] = zero

    @pl.when(sy == 0)
    def _():
        for l in range(levels):
            for i in range(2):
                edge_l[l, i] = zero

    @pl.when(sy == nsy - 1)
    def _():
        for l in range(levels):
            for i in range(2):
                edge_r[l, i] = zero

    r_ids = lax.broadcasted_iota(jnp.int32, (child_cols, child_cols // 3), 0)
    c_ids = lax.broadcasted_iota(jnp.int32, (child_cols, child_cols // 3), 1)
    off = r_ids - 3 * c_ids
    pick = jnp.where((off >= 0) & (off <= 2), 1.0, 0.0).astype(jnp.bfloat16)

    p1 = []
    for m in range(members):
        loads[m].wait()
        y = jnp.dot(
            xbuf[m].reshape(levels * child_rows, child_cols),
            pick,
            preferred_element_type=jnp.float32,
        )
        for c in range(2):
            ybuf[m % 2, c] = y[:, c * LANES : (c + 1) * LANES]
        for i in range(rows):
            for c in range(2):
                total = ybuf[m % 2, c, pl.ds(3 * i, levels, stride=child_rows), :]
                for a in (1, 2):
                    total += ybuf[m % 2, c, pl.ds(3 * i + a, levels, stride=child_rows), :]
                psend[i // 2, m, 2 * c + i % 2] = total
        if m == 0:
            pl.semaphore_wait(barrier, greeted)
        for o in range(1, nmem):
            copy = pltpu.make_async_remote_copy(
                src_ref=psend.at[mem_peers[o], m],
                dst_ref=rbuf.at[o, m],
                send_sem=p1_send.at[o, m],
                recv_sem=p1_recv.at[o, m],
                device_id=at(mem_peers[o], sx, sy),
                device_id_type=MESH,
            )
            copy.start()
            p1.append(copy)
        for v in range(4):
            rbuf[0, m, v] = psend[mem, m, v]
    for copy in p1:
        copy.wait_recv()

    def anomalies(v, var):
        total = zero
        for o in range(nmem):
            for m in range(members):
                total += rbuf[o, m, v]
        mean = total * (1.0 / total_members)
        mbuf[v] = mean * (1.0 / 9.0)
        for o in range(nmem):
            for m in range(members):
                anom = rbuf[o, m, v] - mean
                abuf[v, o * members + m] = anom
                var += anom * anom
        return var

    var = lax.fori_loop(0, 4, anomalies, zero)
    s1[0] = var
    s1_copies = []
    for o in range(1, nmem):
        copy = pltpu.make_async_remote_copy(
            src_ref=s1.at[0],
            dst_ref=s1.at[o],
            send_sem=s1_send.at[o],
            recv_sem=s1_recv.at[o],
            device_id=at(mem_peers[o], sx, sy),
            device_id_type=MESH,
        )
        copy.start()
        s1_copies.append(copy)

    factor = 1.0 / (81.0 * (total_members - 1))

    def covariances(v, carry):
        acc = [zero] * levels
        for t in range(total_members):
            anom = abuf[v, t]
            for l in range(levels):
                acc[l] += anom * abuf[v, t, pl.ds(l, 1), :]
        for l in range(levels):
            msg[l, v] = acc[l] * factor
        return carry

    lax.fori_loop(0, 4, covariances, 0)
    for l in range(levels):
        msg[l, 4] = zero
        for v in range(4):
            msg[l, 4, pl.ds(v, 1), :] = mbuf[v, pl.ds(l, 1), :]

    def to_right():
        return pltpu.make_async_remote_copy(
            src_ref=msg.at[:, pl.ds(2, 2)],
            dst_ref=edge_l,
            send_sem=e_send.at[0],
            recv_sem=e_recv.at[0],
            device_id=at(mem, sx, lax.rem(sy + 1, nsy)),
            device_id_type=MESH,
        )

    def to_left():
        return pltpu.make_async_remote_copy(
            src_ref=msg.at[:, pl.ds(0, 2)],
            dst_ref=edge_r,
            send_sem=e_send.at[1],
            recv_sem=e_recv.at[1],
            device_id=at(mem, sx, lax.rem(sy + nsy - 1, nsy)),
            device_id_type=MESH,
        )

    @pl.when(sy < nsy - 1)
    def _():
        to_right().start()

    @pl.when(sy > 0)
    def _():
        to_left().start()

    def to_owner(src, dst, slot, owner, x, send, recv):
        return pltpu.make_async_remote_copy(
            src_ref=src.at[owner],
            dst_ref=dst.at[slot],
            send_sem=send,
            recv_sem=recv.at[slot],
            device_id=at(owner, x, sy),
            device_id_type=MESH,
        )

    def to_tile(src, dst, send, recv):
        return [
            to_owner(src, dst, mem + 2, mem_peers[o], sx, send.at[o], recv)
            for o in range(1, nmem)
        ]

    def to_low(src, dst, send, recv):
        low = lax.rem(sx + nsx - 1, nsx)
        slot = mem + nmem + 2
        return [to_owner(src, dst, slot, l, low, send.at[l], recv) for l in range(nmem)]

    def to_high(src, dst, send, recv):
        high = lax.rem(sx + 1, nsx)
        slot = mem - (nmem - 2)
        return [to_owner(src, dst, slot, l, high, send.at[l], recv) for l in range(nmem)]

    sends_down = (mem < 2) & (sx > 0)
    sends_up = (mem >= nmem - 2) & (sx < nsx - 1)

    def start_all(src, dst, send_tile, send_next, recv):
        for copy in to_tile(src, dst, send_tile, recv):
            copy.start()
        @pl.when(sends_down)
        def _():
            for copy in to_low(src, dst, send_next, recv):
                copy.start()
        @pl.when(sends_up)
        def _():
            for copy in to_high(src, dst, send_next, recv):
                copy.start()

    start_all(msg, q, q_send, r_send, q_recv)
    for v in range(5):
        q[mem + 2, v] = msg[mem, v]

    @pl.when(sy < nsy - 1)
    def _():
        to_left().wait_recv()

    @pl.when(sy > 0)
    def _():
        to_right().wait_recv()

    lane = lax.broadcasted_iota(jnp.int32, (SUB, LANES), 1)
    low_half = lane < LANES // 2
    for l in range(levels):
        for i in range(2):
            hsend[l, i] = jnp.where(low_half, edge_r[l, i], edge_l[l, i])
    start_all(hsend, h, h_send, g_send, h_recv)
    for v in range(2):
        h[mem + 2, v] = hsend[mem, v]

    for copy in s1_copies:
        copy.wait_recv()
    tile = s1[0]
    for o in range(1, nmem):
        tile += s1[o]
    s2[0] = tile
    s2_copies = []
    for n, (x, y) in enumerate(plane_peers):
        copy = pltpu.make_async_remote_copy(
            src_ref=s2.at[0],
            dst_ref=s2.at[n + 1],
            send_sem=s2_send.at[n + 1],
            recv_sem=s2_recv.at[n + 1],
            device_id=at(mem, x, y),
            device_id_type=MESH,
        )
        copy.start()
        s2_copies.append(copy)

    def arrived(dst, recv, slot):
        pltpu.make_async_remote_copy(
            src_ref=dst.at[slot],
            dst_ref=dst.at[slot],
            send_sem=q_send.at[0],
            recv_sem=recv.at[slot],
            device_id=at(mem_peers[1], sx, sy),
            device_id_type=MESH,
        ).wait_recv()

    for dst, recv in ((q, q_recv), (h, h_recv)):
        for o in range(1, nmem):
            arrived(dst, recv, mem_peers[o] + 2)

        @pl.when(sx > 0)
        def _():
            for slot in range(2):
                arrived(dst, recv, slot)

        @pl.when(sx < nsx - 1)
        def _():
            for slot in range(nmem + 2, nmem + 4):
                arrived(dst, recv, slot)

    for d in range(nmem):
        for i in range(2):
            for c in range(2):
                mean_ref[0, pl.ds(2 * d + i, 1), pl.ds(c * LANES, LANES)] = q[
                    d + 2, 4, pl.ds(2 * c + i, 1), :
                ]

    table = gaspari_table(REACH)

    def cells(i):
        slot, i2 = i // 2, i % 2
        return jnp.concatenate([q[slot, i2], q[slot, 2 + i2], h[slot, i2]], axis=1)

    for i in range(rows):
        center = i + REACH
        lines = [cells(center)]
        for e in range(1, REACH + 1):
            lines.append(cells(center - e) + cells(center + e))
        out = None
        for f in range(REACH + 1):
            line = None
            for e in range(REACH + 1):
                weight = float(table[REACH + e, REACH + f])
                if weight != 0.0:
                    term = weight * lines[e]
                    line = term if line is None else line + term
            if f == 0:
                out = line
            else:
                width = 3 * LANES
                out = out + pltpu.roll(line, f, 1) + pltpu.roll(line, width - f, 1)
        for c in range(2):
            zbuf[c, pl.ds(i, levels, stride=rows), :] = out[:, c * LANES : (c + 1) * LANES]

    for copy in s2_copies:
        copy.wait_recv()
    everyone = s2[0]
    for n in range(len(s2_copies)):
        everyone += s2[n + 1]
    count = levels * rows * nsx * child_cols // 3 * nsy
    spread = jnp.sum(everyone, keepdims=True) * (factor / count)
    scale = 1.0 / (spread + 1e-6)
    for k in range(levels):
        for c in range(2):
            cov_ref[k, :, pl.ds(c * LANES, LANES)] = zbuf[c, pl.ds(k * rows, rows), :] * scale

    for copy in p1 + s1_copies + s2_copies:
        copy.wait_send()
    for src, dst, tile_sem, next_sem, recv in (
        (msg, q, q_send, r_send, q_recv),
        (hsend, h, h_send, g_send, h_recv),
    ):
        for copy in to_tile(src, dst, tile_sem, recv):
            copy.wait_send()

        @pl.when(sends_down)
        def _():
            for copy in to_low(src, dst, next_sem, recv):
                copy.wait_send()

        @pl.when(sends_up)
        def _():
            for copy in to_high(src, dst, next_sem, recv):
                copy.wait_send()

    @pl.when(sy < nsy - 1)
    def _():
        to_right().wait_send()

    @pl.when(sy > 0)
    def _():
        to_left().wait_send()


def solution(mesh):
    nmem, nsx, nsy = (mesh.shape[name] for name in ("mem", "sx", "sy"))

    def local(child):
        members, levels, child_rows, child_cols = child.shape
        rows, cols = child_rows // 3, child_cols // 3
        f32 = jnp.float32
        dma = pltpu.SemaphoreType.DMA
        return pl.pallas_call(
            functools.partial(kernel, nmem, nsx, nsy),
            out_shape=(
                jax.ShapeDtypeStruct((levels // nmem, rows, cols), f32),
                jax.ShapeDtypeStruct((levels, rows, cols), f32),
            ),
            in_specs=[pl.BlockSpec(memory_space=pl.ANY)],
            out_specs=(
                pl.BlockSpec(memory_space=pltpu.VMEM),
                pl.BlockSpec(memory_space=pltpu.VMEM),
            ),
            scratch_shapes=[
                pltpu.VMEM(child.shape, child.dtype),
                pltpu.VMEM((2, 2, levels * child_rows, LANES), f32),
                pltpu.VMEM((nmem, members, 4, SUB, LANES), f32),
                pltpu.VMEM((nmem, members, 4, SUB, LANES), f32),
                pltpu.VMEM((4, nmem * members, SUB, LANES), f32),
                pltpu.VMEM((4, SUB, LANES), f32),
                pltpu.VMEM((levels, 5, SUB, LANES), f32),
                pltpu.VMEM((nmem + 4, 5, SUB, LANES), f32),
                pltpu.VMEM((levels, 2, SUB, LANES), f32),
                pltpu.VMEM((levels, 2, SUB, LANES), f32),
                pltpu.VMEM((levels, 2, SUB, LANES), f32),
                pltpu.VMEM((nmem + 4, 2, SUB, LANES), f32),
                pltpu.VMEM((2, levels * rows, LANES), f32),
                pltpu.VMEM((nmem, SUB, LANES), f32),
                pltpu.VMEM((nsx * nsy, SUB, LANES), f32),
                dma((members,)),
                dma((nmem, members)),
                dma((nmem, members)),
                dma((nmem,)),
                dma((nmem,)),
                dma((2,)),
                dma((2,)),
                dma((nmem,)),
                dma((nmem + 4,)),
                dma((nmem,)),
                dma((nmem,)),
                dma((nmem + 4,)),
                dma((nmem,)),
                dma((nsx * nsy,)),
                dma((nsx * nsy,)),
            ],
            compiler_params=pltpu.CompilerParams(collective_id=0, has_side_effects=True),
        )(child)

    return jax.shard_map(
        local,
        mesh=mesh,
        in_specs=(P("mem", None, "sx", "sy"),),
        out_specs=(P("mem", "sx", "sy"), P("mem", "sx", "sy")),
        check_vma=False,
    )
```

```python
import functools

import jax
import jax.numpy as jnp
import numpy as np
from jax import lax
from jax.experimental import pallas as pl
from jax.experimental.pallas import tpu as pltpu
from jax.sharding import PartitionSpec as P

MESH = pl.DeviceIdType.MESH
REACH = 4
LANES = 128
SUB = 8
VMEM_GRANT = 55_500_000


def gaspari_table(reach):
    offsets = np.arange(-reach, reach + 1) * 1.0
    dist = np.sqrt(offsets[:, None] ** 2 + offsets[None, :] ** 2) / 2.5
    near = -0.25 * dist**5 + 0.5 * dist**4 + 0.625 * dist**3 - 5.0 / 3.0 * dist**2 + 1.0
    safe = np.maximum(dist, 0.001)
    far = (
        dist**5 / 12.0
        - 0.5 * dist**4
        + 0.625 * dist**3
        + 5.0 / 3.0 * dist**2
        - 5.0 * dist
        + 4.0
        - 2.0 / (3.0 * safe)
    )
    table = np.where(dist <= 1.0, near, np.where(dist < 2.0, far, 0.0))
    return table / table.sum()


def gather(
    nmem,
    nsx,
    nsy,
    child_ref,
    z_ref,
    all_ref,
    means_ref,
    xbuf,
    ybuf,
    psend,
    rbuf,
    pack,
    from_left,
    from_right,
    hsend,
    hbuf,
    abuf,
    mbuf,
    mmsg,
    means,
    msg,
    q,
    odd,
    s1,
    s2,
    ld_sem,
    p1_sem,
    e_send,
    e_recv,
    h_sem,
    s1_sem,
    m_sem,
    q_sem,
    n_send,
    n_recv,
    s2_sem,
):
    members, levels, child_rows, child_cols = child_ref.shape
    rows = child_rows // 3
    mem = lax.axis_index("mem")
    sx = lax.axis_index("sx")
    sy = lax.axis_index("sy")
    total_members = members * nmem
    here = {"mem": mem, "sx": sx, "sy": sy}

    loads = []
    for m in range(members):
        copy = pltpu.make_async_copy(child_ref.at[m], xbuf.at[m], ld_sem.at[m])
        copy.start()
        loads.append(copy)

    ring = nmem // 2
    z, y = mem // ring, lax.rem(mem, ring)
    steps = [(a, b) for b in (2, 1, 3, 0) for a in range(2) if (a, b) != (0, 0)]
    peers = [lax.rem(z + a, 2) * ring + lax.rem(y + b, ring) for a, b in steps]
    plane = [(a, b) for a in range(nsx) for b in range(nsy) if (a, b) != (0, 0)]
    plane_peers = [(lax.rem(sx + a, nsx), lax.rem(sy + b, nsy)) for a, b in plane]
    above, below = lax.rem(sx + 1, nsx), lax.rem(sx + nsx - 1, nsx)

    def at(m=None, x=None, y=None):
        return {
            "mem": here["mem"] if m is None else m,
            "sx": here["sx"] if x is None else x,
            "sy": here["sy"] if y is None else y,
        }

    def send(src, dst, pair, device):
        copy = pltpu.make_async_remote_copy(
            src_ref=src,
            dst_ref=dst,
            send_sem=pair[0],
            recv_sem=pair[1],
            device_id=device,
            device_id_type=MESH,
        )
        copy.start()

    def settle(ref, sem, received):
        copy = pltpu.make_async_remote_copy(
            src_ref=ref,
            dst_ref=ref,
            send_sem=sem,
            recv_sem=sem,
            device_id=at(m=peers[0]),
            device_id_type=MESH,
        )
        if received:
            copy.wait_recv()
        else:
            copy.wait_send()

    barrier = pltpu.get_barrier_semaphore()
    friends = [at(m=p) for p in peers]
    friends += [at(x=a, y=b) for a, b in plane_peers]
    friends += [at(m=p, x=x) for p in peers for x in (above, below)]
    for friend in friends:
        pl.semaphore_signal(barrier, inc=1, device_id=friend, device_id_type=MESH)

    zero = jnp.zeros((SUB, LANES), jnp.float32)

    def clear_slots(first):
        for slot in range(first, first + 2):
            for v in range(5):
                q[slot, v] = zero

    def clear_side(ref):
        for d in range(nmem):
            ref[d] = zero

    pl.when(sx == 0)(lambda: clear_slots(0))
    pl.when(sx == nsx - 1)(lambda: clear_slots(nmem + 2))
    pl.when(sy == 0)(lambda: clear_side(from_left))
    pl.when(sy == nsy - 1)(lambda: clear_side(from_right))

    r_ids = lax.broadcasted_iota(jnp.int32, (child_cols, child_cols // 3), 0)
    c_ids = lax.broadcasted_iota(jnp.int32, (child_cols, child_cols // 3), 1)
    off = r_ids - 3 * c_ids
    pick = jnp.where((off >= 0) & (off <= 2), 1.0, 0.0).astype(jnp.bfloat16)

    for m in range(members):
        loads[m].wait()
        wide = jnp.dot(
            xbuf[m].reshape(levels * child_rows, child_cols),
            pick,
            preferred_element_type=jnp.float32,
        )
        for c in range(2):
            ybuf[m % 2, c] = wide[:, c * LANES : (c + 1) * LANES]
        for i in range(rows):
            for c in range(2):
                total = ybuf[m % 2, c, pl.ds(3 * i, levels, stride=child_rows), :]
                for a in (1, 2):
                    total += ybuf[m % 2, c, pl.ds(3 * i + a, levels, stride=child_rows), :]
                psend[i // 2, m, 2 * c + i % 2] = total
        if m == 0:
            pl.semaphore_wait(barrier, len(friends))
        for n, p in enumerate(peers):
            send(psend.at[p, m], rbuf.at[n + 1, m], (p1_sem.at[0], p1_sem.at[1]), at(m=p))
        for v in range(4):
            rbuf[0, m, v] = psend[mem, m, v]

    lane = lax.broadcasted_iota(jnp.int32, (SUB, LANES), 1)
    for d in range(nmem):
        packed = zero
        for m in range(members):
            for i in range(2):
                shift = 8 * m + 64 * i
                both = jnp.where(lane < LANES // 2, psend[d, m, i], psend[d, m, 2 + i])
                if shift:
                    both = pltpu.roll(both, shift, 1)
                mine = ((lane - shift + 4 + LANES) & (LANES - 1)) < 8
                packed = jnp.where(mine, both, packed)
        pack[d] = packed

    @pl.when(sy < nsy - 1)
    def _():
        send(pack, from_left, (e_send.at[0], e_recv.at[0]), at(y=lax.rem(sy + 1, nsy)))

    @pl.when(sy > 0)
    def _():
        send(pack, from_right, (e_send.at[1], e_recv.at[1]), at(y=lax.rem(sy + nsy - 1, nsy)))

    pl.when(sy > 0)(lambda: settle(from_left, e_recv.at[0], True))
    pl.when(sy < nsy - 1)(lambda: settle(from_right, e_recv.at[1], True))
    for d in range(nmem):
        hsend[d] = jnp.where((lane & 4) == 0, from_right[d], from_left[d])
    for n, p in enumerate(peers):
        send(hsend.at[p], hbuf.at[n + 1], (h_sem.at[0], h_sem.at[1]), at(m=p))
    hbuf[0] = hsend[mem]

    settle(rbuf.at[pl.ds(1, nmem - 1)], p1_sem.at[1], True)

    def anomalies(v, var):
        total = zero
        for o in range(nmem):
            for m in range(members):
                total += rbuf[o, m, v]
        mean = total * (1.0 / total_members)
        mbuf[v] = mean * (1.0 / 9.0)
        for o in range(nmem):
            for m in range(members):
                anom = rbuf[o, m, v] - mean
                abuf[v, o * members + m] = anom
                var += anom * anom
        return var

    var = lax.fori_loop(0, 4, anomalies, zero)
    s1[0] = var
    for n, p in enumerate(peers):
        send(s1.at[0], s1.at[n + 1], (s1_sem.at[0], s1_sem.at[1]), at(m=p))
    for l in range(levels):
        mmsg[l] = zero
        for v in range(4):
            mmsg[l, pl.ds(v, 1), :] = mbuf[v, pl.ds(l, 1), :]
    for p in peers:
        send(mmsg.at[p], means.at[mem], (m_sem.at[0], m_sem.at[1]), at(m=p))
    means[mem] = mmsg[mem]

    settle(hbuf.at[pl.ds(1, nmem - 1)], h_sem.at[1], True)
    total = zero
    for o in range(nmem):
        for m in range(members):
            value = pltpu.roll(hbuf[o], LANES - 8 * m, 1) if m else hbuf[o]
            abuf[4, o * members + m] = value
            total += value
    mean = total * (1.0 / total_members)
    for t in range(total_members):
        abuf[4, t] = abuf[4, t] - mean

    factor = 1.0 / (81.0 * (total_members - 1))

    def covariances(v, carry):
        acc = [zero] * levels
        for t in range(total_members):
            anom = abuf[v, t]
            for l in range(levels):
                acc[l] += anom * abuf[v, t, pl.ds(l, 1), :]
        for l in range(levels):
            msg[l, v] = acc[l] * factor
        return carry

    lax.fori_loop(0, 5, covariances, 0)

    for p in peers:
        send(msg.at[p], q.at[mem + 2], (q_sem.at[0], q_sem.at[1]), at(m=p))
    sends_down = (mem < 2) & (sx > 0)
    sends_up = (mem >= nmem - 2) & (sx < nsx - 1)

    @pl.when(sends_down)
    def _():
        for l in range(levels):
            send(msg.at[l], q.at[mem + nmem + 2], (n_send.at[0], n_recv.at[1]), at(m=l, x=below))

    @pl.when(sends_up)
    def _():
        for l in range(levels):
            send(msg.at[l], q.at[mem - nmem + 2], (n_send.at[0], n_recv.at[0]), at(m=l, x=above))

    for v in range(5):
        q[mem + 2, v] = msg[mem, v]

    settle(s1.at[pl.ds(1, nmem - 1)], s1_sem.at[1], True)
    tile = s1[0]
    for o in range(1, nmem):
        tile += s1[o]
    s2[0] = tile
    for n, (a, b) in enumerate(plane_peers):
        send(s2.at[0], s2.at[n + 1], (s2_sem.at[0], s2_sem.at[1]), at(x=a, y=b))

    settle(means.at[pl.ds(0, nmem - 1)], m_sem.at[1], True)
    for d in range(nmem):
        means_ref[d] = means[d]
    settle(q.at[pl.ds(0, nmem - 1)], q_sem.at[1], True)
    pl.when(sx > 0)(lambda: settle(q.at[pl.ds(0, 2)], n_recv.at[0], True))
    pl.when(sx < nsx - 1)(lambda: settle(q.at[pl.ds(nmem + 2, 2)], n_recv.at[1], True))

    table = gaspari_table(REACH)

    for slot in range(nmem + 4):
        odd[slot] = pltpu.roll(q[slot, 4], LANES // 2, 1)

    def cells(i):
        slot, i2 = i // 2, i % 2
        side = odd[slot] if i2 else q[slot, 4]
        return jnp.concatenate([q[slot, i2], q[slot, 2 + i2], side], axis=1)

    for i in range(rows):
        center = i + REACH
        lines = [cells(center)]
        for e in range(1, REACH + 1):
            lines.append(cells(center - e) + cells(center + e))
        out = None
        for f in range(REACH + 1):
            line = None
            for e in range(REACH + 1):
                weight = float(table[REACH + e, REACH + f])
                if weight != 0.0:
                    term = weight * lines[e]
                    line = term if line is None else line + term
            if f == 0:
                out = line
            else:
                width = 3 * LANES
                out = out + pltpu.roll(line, f, 1) + pltpu.roll(line, width - f, 1)
        for c in range(2):
            z_ref[c, pl.ds(i, levels, stride=rows), :] = out[:, c * LANES : (c + 1) * LANES]

    settle(s2.at[pl.ds(1, len(plane))], s2_sem.at[1], True)
    everyone = s2[0]
    for n in range(len(plane)):
        everyone += s2[n + 1]
    all_ref[...] = everyone

    settle(psend.at[pl.ds(0, nmem - 1)], p1_sem.at[0], False)
    pl.when(sy < nsy - 1)(lambda: settle(pack, e_send.at[0], False))
    pl.when(sy > 0)(lambda: settle(pack, e_send.at[1], False))
    settle(hsend.at[pl.ds(0, nmem - 1)], h_sem.at[0], False)
    settle(s1.at[pl.ds(0, nmem - 1)], s1_sem.at[0], False)
    settle(mmsg.at[pl.ds(0, nmem - 1)], m_sem.at[0], False)
    settle(msg.at[pl.ds(0, nmem - 1)], q_sem.at[0], False)
    pl.when(sends_down | sends_up)(lambda: settle(msg, n_send.at[0], False))
    settle(s2.at[pl.ds(0, len(plane))], s2_sem.at[0], False)


def scale(count, z_ref, all_ref, means_ref, mean_ref, cov_ref):
    levels, rows, cols = cov_ref.shape
    spread = jnp.sum(all_ref[...], keepdims=True) * (1.0 / count)
    inverse = 1.0 / (spread + 1e-6)
    for k in range(levels):
        for c in range(cols // LANES):
            block = z_ref[c, pl.ds(k * rows, rows), :]
            cov_ref[k, :, pl.ds(c * LANES, LANES)] = block * inverse
    for i in range(rows):
        for c in range(cols // LANES):
            row = means_ref[i // 2, pl.ds(2 * c + i % 2, 1), :]
            mean_ref[0, pl.ds(i, 1), pl.ds(c * LANES, LANES)] = row


def solution(mesh):
    nmem, nsx, nsy = (mesh.shape[name] for name in ("mem", "sx", "sy"))

    def local(child):
        members, levels, child_rows, child_cols = child.shape
        rows, cols = child_rows // 3, child_cols // 3
        f32 = jnp.float32
        dma = pltpu.SemaphoreType.DMA
        vmem = pl.BlockSpec(memory_space=pltpu.VMEM)
        vector = (SUB, LANES)
        z, total, means = pl.pallas_call(
            functools.partial(gather, nmem, nsx, nsy),
            out_shape=(
                jax.ShapeDtypeStruct((2, levels * rows, LANES), f32),
                jax.ShapeDtypeStruct(vector, f32),
                jax.ShapeDtypeStruct((nmem, *vector), f32),
            ),
            in_specs=[pl.BlockSpec(memory_space=pltpu.MemorySpace.HBM)],
            out_specs=(vmem, vmem, vmem),
            scratch_shapes=[
                pltpu.VMEM(child.shape, child.dtype),
                pltpu.VMEM((2, 2, levels * child_rows, LANES), f32),
                pltpu.VMEM((nmem, members, 4, *vector), f32),
                pltpu.VMEM((nmem, members, 4, *vector), f32),
                pltpu.VMEM((nmem, *vector), f32),
                pltpu.VMEM((nmem, *vector), f32),
                pltpu.VMEM((nmem, *vector), f32),
                pltpu.VMEM((nmem, *vector), f32),
                pltpu.VMEM((nmem, *vector), f32),
                pltpu.VMEM((5, nmem * members, *vector), f32),
                pltpu.VMEM((4, *vector), f32),
                pltpu.VMEM((levels, *vector), f32),
                pltpu.VMEM((nmem, *vector), f32),
                pltpu.VMEM((levels, 5, *vector), f32),
                pltpu.VMEM((nmem + 4, 5, *vector), f32),
                pltpu.VMEM((nmem + 4, *vector), f32),
                pltpu.VMEM((nmem, *vector), f32),
                pltpu.VMEM((nsx * nsy, *vector), f32),
                dma((members,)),
                dma((2,)),
                dma((2,)),
                dma((2,)),
                dma((2,)),
                dma((2,)),
                dma((2,)),
                dma((2,)),
                dma((1,)),
                dma((2,)),
                dma((2,)),
            ],
            compiler_params=pltpu.CompilerParams(collective_id=0, has_side_effects=True, vmem_limit_bytes=VMEM_GRANT),
            name="gather",
        )(child)
        count = 81.0 * (members * nmem - 1) * levels * rows * nsx * cols * nsy
        return pl.pallas_call(
            functools.partial(scale, count),
            out_shape=(
                jax.ShapeDtypeStruct((levels // nmem, rows, cols), f32),
                jax.ShapeDtypeStruct((levels, rows, cols), f32),
            ),
            in_specs=[vmem, vmem, vmem],
            out_specs=(vmem, vmem),
            compiler_params=pltpu.CompilerParams(vmem_limit_bytes=8 << 20),
            name="scale",
        )(z, total, means)

    return jax.shard_map(
        local,
        mesh=mesh,
        in_specs=(P("mem", None, "sx", "sy"),),
        out_specs=(P("mem", "sx", "sy"), P("mem", "sx", "sy")),
        check_vma=False,
    )
```

```python
import functools

import jax
import jax.numpy as jnp
import numpy as np
from jax import lax
from jax.experimental import pallas as pl
from jax.experimental.pallas import tpu as pltpu
from jax.sharding import PartitionSpec as P

MESH = pl.DeviceIdType.MESH
REACH = 4
LANES = 128
SUB = 8
VMEM_GRANT = 55_500_000


def gaspari_table(reach):
    offsets = np.arange(-reach, reach + 1) * 1.0
    dist = np.sqrt(offsets[:, None] ** 2 + offsets[None, :] ** 2) / 2.5
    near = -0.25 * dist**5 + 0.5 * dist**4 + 0.625 * dist**3 - 5.0 / 3.0 * dist**2 + 1.0
    safe = np.maximum(dist, 0.001)
    far = (
        dist**5 / 12.0
        - 0.5 * dist**4
        + 0.625 * dist**3
        + 5.0 / 3.0 * dist**2
        - 5.0 * dist
        + 4.0
        - 2.0 / (3.0 * safe)
    )
    table = np.where(dist <= 1.0, near, np.where(dist < 2.0, far, 0.0))
    return table / table.sum()


def gather(
    nmem,
    nsx,
    nsy,
    child_ref,
    z_ref,
    all_ref,
    means_ref,
    xbuf,
    pick,
    ybuf,
    psend,
    rbuf,
    pack,
    from_left,
    from_right,
    hsend,
    hbuf,
    abuf,
    sbuf,
    mbuf,
    mmsg,
    means,
    msg,
    q,
    odd,
    s1,
    s2,
    ld_sem,
    p1_sem,
    e_send,
    e_recv,
    h_sem,
    s1_sem,
    m_sem,
    q_sem,
    n_send,
    n_recv,
    s2_sem,
):
    members, levels, child_rows, child_cols = child_ref.shape
    rows = child_rows // 3
    half_rows = child_rows // 2
    mem = lax.axis_index("mem")
    sx = lax.axis_index("sx")
    sy = lax.axis_index("sy")
    total_members = members * nmem
    ring = nmem // 2
    z, y = mem // ring, lax.rem(mem, ring)

    def at(m=None, x=None, y=None):
        return {
            "mem": mem if m is None else m,
            "sx": sx if x is None else x,
            "sy": sy if y is None else y,
        }

    loads = []
    for half, owner_z in enumerate((1 - z, z)):
        first = pl.multiple_of(owner_z * half_rows, SUB)
        copy = pltpu.make_async_copy(
            child_ref.at[:, :, pl.ds(first, half_rows), :], xbuf.at[half], ld_sem.at[half]
        )
        copy.start()
        loads.append(copy)

    steps = [(1, 0), (1, 1), (1, 3), (1, 2), (0, 2), (0, 1), (0, 3)]
    spots = [lax.rem(y + b, ring) for _, b in steps]
    peers = [lax.rem(z + a, 2) * ring + spot for (a, _), spot in zip(steps, spots)]
    plane = [(a, b) for a in range(nsx) for b in range(nsy) if (a, b) != (0, 0)]
    plane_peers = [(lax.rem(sx + a, nsx), lax.rem(sy + b, nsy)) for a, b in plane]
    above, below = lax.rem(sx + 1, nsx), lax.rem(sx + nsx - 1, nsx)

    def send(src, dst, pair, device):
        copy = pltpu.make_async_remote_copy(
            src_ref=src,
            dst_ref=dst,
            send_sem=pair[0],
            recv_sem=pair[1],
            device_id=device,
            device_id_type=MESH,
        )
        copy.start()

    def settle(ref, sem, received):
        copy = pltpu.make_async_remote_copy(
            src_ref=ref,
            dst_ref=ref,
            send_sem=sem,
            recv_sem=sem,
            device_id=at(m=peers[0]),
            device_id_type=MESH,
        )
        if received:
            copy.wait_recv()
        else:
            copy.wait_send()

    barrier = pltpu.get_barrier_semaphore()
    friends = [at(m=p) for p in peers]
    friends += [at(x=a, y=b) for a, b in plane_peers]
    friends += [at(m=p, x=x) for p in peers for x in (above, below)]
    for friend in friends:
        pl.semaphore_signal(barrier, inc=1, device_id=friend, device_id_type=MESH)

    zero = jnp.zeros((SUB, LANES), jnp.float32)

    width = 3 * LANES
    r_ids = lax.broadcasted_iota(jnp.int32, (width, LANES), 0)
    c_ids = lax.broadcasted_iota(jnp.int32, (width, LANES), 1)
    off = r_ids - 3 * c_ids
    pick[...] = jnp.where((off >= 0) & (off <= 2), 1.0, 0.0).astype(jnp.bfloat16)

    def post(first, count, n, sem):
        part = pl.ds(first, count)
        send(
            psend.at[1 - steps[n][0], spots[n], part],
            rbuf.at[n + 1, part],
            (p1_sem.at[0], p1_sem.at[sem]),
            at(m=peers[n]),
        )

    within = zero
    for half, owner_z in enumerate((1 - z, z)):
        loads[half].wait()
        for c in range(2):
            ybuf[c] = jnp.dot(
                xbuf[half, :, :, :, pl.ds(c * width, width)].reshape(-1, width),
                pick[...],
                preferred_element_type=jnp.float32,
            )
        for i in range(rows // 2):
            for c in range(2):
                p = []
                for m in range(members):
                    total = None
                    for a in range(3):
                        start = m * levels * half_rows + 3 * i + a
                        line = ybuf[c, pl.ds(start, levels, stride=half_rows), :]
                        total = line if total is None else total + line
                    p.append(total)
                up, down = p[0] + p[1], p[2] + p[3]
                left, right = p[0] - p[1], p[2] - p[3]
                owner, inside = i % ring, i // ring
                i2 = inside + owner_z - 2 * inside * owner_z
                psend[half, owner, 2 * i2 + c] = up + down
                for j, value in enumerate((up - down, left + right, left - right)):
                    psend[half, owner, 4 + 6 * i2 + 2 * j + c] = value
                    within += value * value
        if half == 0:
            pl.semaphore_wait(barrier, len(friends))
            for n in range(ring):
                post(0, 4, n, 1)
            post(4, 6, 0, 2)
        else:
            for n in range(ring, nmem - 1):
                post(0, 4, n, 1)
            for n in range(1, nmem - 1):
                post(4, 6, n, 2)
    for k in range(16):
        rbuf[0, k] = psend[1, y, k]

    def clear_rows(first):
        for row in range(first, first + REACH):
            for v in range(3):
                q[row, v] = zero

    def clear_side(ref):
        for d in range(nmem):
            ref[d] = zero

    pl.when(sx == 0)(lambda: clear_rows(0))
    pl.when(sx == nsx - 1)(lambda: clear_rows(REACH + rows))
    pl.when(sy == 0)(lambda: clear_side(from_left))
    pl.when(sy == nsy - 1)(lambda: clear_side(from_right))

    lane = lax.broadcasted_iota(jnp.int32, (SUB, LANES), 1)
    for d in range(nmem):
        half, owner = d // ring, d % ring
        packed = zero
        for j in range(members):
            for i2 in range(2):
                shift = 8 * j + 64 * i2
                k = 2 * i2 if j == 0 else 2 + 6 * i2 + 2 * j
                both = jnp.where(
                    lane < LANES // 2, psend[half, owner, k], psend[half, owner, k + 1]
                )
                if shift:
                    both = pltpu.roll(both, shift, 1)
                mine = ((lane - shift + 4 + LANES) & (LANES - 1)) < 8
                packed = jnp.where(mine, both, packed)
        pack[d] = packed

    @pl.when(sy < nsy - 1)
    def _():
        send(pack, from_left, (e_send.at[0], e_recv.at[0]), at(y=lax.rem(sy + 1, nsy)))

    @pl.when(sy > 0)
    def _():
        send(pack, from_right, (e_send.at[1], e_recv.at[1]), at(y=lax.rem(sy + nsy - 1, nsy)))

    pl.when(sy > 0)(lambda: settle(from_left, e_recv.at[0], True))
    pl.when(sy < nsy - 1)(lambda: settle(from_right, e_recv.at[1], True))
    for d in range(nmem):
        hsend[d] = jnp.where((lane & 4) == 0, from_right[d], from_left[d])
    for n, (p, spot) in enumerate(zip(peers, spots)):
        send(
            hsend.at[(1 - steps[n][0]) * ring + spot],
            hbuf.at[n + 1],
            (h_sem.at[0], h_sem.at[1]),
            at(m=p),
        )
    hbuf[0] = hsend[ring + y]

    settle(rbuf.at[pl.ds(1, nmem - 1), pl.ds(0, 4)], p1_sem.at[1], True)
    var = within
    for v in range(4):
        total = rbuf[0, v]
        for o in range(1, nmem):
            total += rbuf[o, v]
        mbuf[v] = total * (1.0 / (9.0 * total_members))
        middle = total * (1.0 / nmem)
        for o in range(nmem):
            anom = rbuf[o, v] - middle
            abuf[v, o] = anom
            var += anom * anom
    s1[0] = var
    for n, p in enumerate(peers):
        send(s1.at[0], s1.at[n + 1], (s1_sem.at[0], s1_sem.at[1]), at(m=p))
    for n in range(nmem - 1):
        post(10, 6, n, 3)
    for l in range(levels):
        mmsg[l] = zero
        for v in range(4):
            mmsg[l, pl.ds(v, 1), :] = mbuf[v, pl.ds(l, 1), :]
    for p in peers:
        send(mmsg.at[p], means.at[mem], (m_sem.at[0], m_sem.at[1]), at(m=p))
    means[mem] = mmsg[mem]

    factor = 1.0 / (4.0 * 81.0 * (total_members - 1))

    def covariances(v, vectors):
        acc = [zero] * levels
        for ref, index in vectors:
            anom = ref[index]
            for l in range(levels):
                acc[l] += anom * ref[(*index, pl.ds(l, 1), slice(None))]
        for l in range(levels):
            msg[l, v] = acc[l] * factor

    def cells_of_row(i2, first):
        def column(c, carry):
            vectors = []
            for o in range(nmem):
                vectors.append((abuf, (2 * i2 + c, o)))
                vectors += [(rbuf, (o, 4 + 6 * i2 + 2 * j + c)) for j in range(members - 1)]
            covariances(first + c, vectors)
            return carry

        lax.fori_loop(0, 2, column, 0)

    settle(rbuf.at[pl.ds(1, nmem - 1), pl.ds(4, 6)], p1_sem.at[2], True)
    cells_of_row(0, 0)
    settle(hbuf.at[pl.ds(1, nmem - 1)], h_sem.at[1], True)
    total = hbuf[0]
    for o in range(1, nmem):
        total += hbuf[o]
    middle = total * (1.0 / nmem)
    for o in range(nmem):
        sbuf[members * o] = hbuf[o] - middle
        for j in range(1, members):
            sbuf[members * o + j] = pltpu.roll(hbuf[o], LANES - 8 * j, 1)
    covariances(2, [(sbuf, (t,)) for t in range(total_members)])

    edge_row = mem + z * (rows - nmem)
    sends_down = (z == 0) & (sx > 0)
    sends_up = (z == 1) & (sx < nsx - 1)
    edge_part, inner_part = pl.ds(0, 3), pl.ds(3, 2)

    @pl.when(sends_down)
    def _():
        for l in range(levels):
            pair = (n_send.at[0], n_recv.at[1])
            row = REACH + rows + mem
            send(msg.at[l, edge_part], q.at[row], pair, at(m=l, x=below))

    @pl.when(sends_up)
    def _():
        for l in range(levels):
            pair = (n_send.at[0], n_recv.at[0])
            row = mem - ring
            send(msg.at[l, edge_part], q.at[row], pair, at(m=l, x=above))

    for p in peers:
        pair = (q_sem.at[0], q_sem.at[1])
        send(msg.at[p, edge_part], q.at[REACH + edge_row], pair, at(m=p))
    for v in range(3):
        q[REACH + edge_row, v] = msg[mem, v]

    settle(s1.at[pl.ds(1, nmem - 1)], s1_sem.at[1], True)
    tile = s1[0]
    for o in range(1, nmem):
        tile += s1[o]
    s2[0] = tile
    for n, (a, b) in enumerate(plane_peers):
        send(s2.at[0], s2.at[n + 1], (s2_sem.at[0], s2_sem.at[1]), at(x=a, y=b))

    settle(rbuf.at[pl.ds(1, nmem - 1), pl.ds(10, 6)], p1_sem.at[3], True)
    cells_of_row(1, 3)
    inner_row = REACH + mem
    for p in peers:
        pair = (q_sem.at[0], q_sem.at[1])
        send(msg.at[p, inner_part], q.at[REACH + inner_row, pl.ds(0, 2)], pair, at(m=p))
    for v in range(2):
        q[REACH + inner_row, v] = msg[mem, 3 + v]

    settle(means.at[pl.ds(0, nmem - 1)], m_sem.at[1], True)
    for d in range(nmem):
        means_ref[d] = means[d]
    settle(msg.at[pl.ds(0, nmem - 1)], q_sem.at[1], True)
    pl.when(sx > 0)(lambda: settle(q.at[pl.ds(0, REACH)], n_recv.at[0], True))
    pl.when(sx < nsx - 1)(lambda: settle(q.at[pl.ds(REACH + rows, REACH)], n_recv.at[1], True))

    table = gaspari_table(REACH)
    for d in range(nmem):
        row = d if d < ring else d + rows - nmem
        odd[d] = pltpu.roll(q[REACH + row, 2], LANES // 2, 1)

    def cells(row):
        inner = row - 2 * REACH
        side = odd[inner] if 0 <= inner < nmem else q[row, 2]
        return jnp.concatenate([q[row, 0], q[row, 1], side], axis=1)

    for i in range(rows):
        center = i + REACH
        lines = [cells(center)]
        for e in range(1, REACH + 1):
            lines.append(cells(center - e) + cells(center + e))
        out = None
        for f in range(REACH + 1):
            line = None
            for e in range(REACH + 1):
                weight = float(table[REACH + e, REACH + f])
                if weight != 0.0:
                    term = weight * lines[e]
                    line = term if line is None else line + term
            if f == 0:
                out = line
            else:
                out = out + pltpu.roll(line, f, 1) + pltpu.roll(line, width - f, 1)
        for c in range(2):
            z_ref[c, pl.ds(i, levels, stride=rows), :] = out[:, c * LANES : (c + 1) * LANES]

    settle(s2.at[pl.ds(1, len(plane))], s2_sem.at[1], True)
    everyone = s2[0]
    for n in range(len(plane)):
        everyone += s2[n + 1]
    all_ref[...] = everyone

    settle(rbuf.at[pl.ds(1, nmem - 1)], p1_sem.at[0], False)
    pl.when(sy < nsy - 1)(lambda: settle(pack, e_send.at[0], False))
    pl.when(sy > 0)(lambda: settle(pack, e_send.at[1], False))
    settle(hsend.at[pl.ds(0, nmem - 1)], h_sem.at[0], False)
    settle(s1.at[pl.ds(0, nmem - 1)], s1_sem.at[0], False)
    settle(mmsg.at[pl.ds(0, nmem - 1)], m_sem.at[0], False)
    settle(msg.at[pl.ds(0, nmem - 1)], q_sem.at[0], False)
    pl.when(sends_down | sends_up)(lambda: settle(q.at[pl.ds(0, levels)], n_send.at[0], False))
    settle(s2.at[pl.ds(0, len(plane))], s2_sem.at[0], False)


def scale(count, z_ref, all_ref, means_ref, mean_ref, cov_ref):
    levels, rows, cols = cov_ref.shape
    spread = jnp.sum(all_ref[...], keepdims=True) * (1.0 / count)
    inverse = 1.0 / (spread + 1e-6)
    for k in range(levels):
        for c in range(cols // LANES):
            block = z_ref[c, pl.ds(k * rows, rows), :]
            cov_ref[k, :, pl.ds(c * LANES, LANES)] = block * inverse
    for i in range(rows):
        inner = 1 if REACH <= i < rows - REACH else 0
        source = i - REACH if inner else i % (rows - 2 * REACH)
        for c in range(cols // LANES):
            row = means_ref[source, pl.ds(2 * inner + c, 1), :]
            mean_ref[0, pl.ds(i, 1), pl.ds(c * LANES, LANES)] = row


def solution(mesh):
    nmem, nsx, nsy = (mesh.shape[name] for name in ("mem", "sx", "sy"))

    def local(child):
        members, levels, child_rows, child_cols = child.shape
        rows, cols = child_rows // 3, child_cols // 3
        f32 = jnp.float32
        dma = pltpu.SemaphoreType.DMA
        vmem = pl.BlockSpec(memory_space=pltpu.VMEM)
        vector = (SUB, LANES)
        z, total, means = pl.pallas_call(
            functools.partial(gather, nmem, nsx, nsy),
            out_shape=(
                jax.ShapeDtypeStruct((2, levels * rows, LANES), f32),
                jax.ShapeDtypeStruct(vector, f32),
                jax.ShapeDtypeStruct((nmem, *vector), f32),
            ),
            in_specs=[pl.BlockSpec(memory_space=pltpu.MemorySpace.HBM)],
            out_specs=(vmem, vmem, vmem),
            scratch_shapes=[
                pltpu.VMEM((2, members, levels, child_rows // 2, child_cols), child.dtype),
                pltpu.VMEM((3 * LANES, LANES), child.dtype),
                pltpu.VMEM((2, members * levels * child_rows // 2, LANES), f32),
                pltpu.VMEM((2, nmem // 2, 16, *vector), f32),
                pltpu.VMEM((nmem, 16, *vector), f32),
                pltpu.VMEM((nmem, *vector), f32),
                pltpu.VMEM((nmem, *vector), f32),
                pltpu.VMEM((nmem, *vector), f32),
                pltpu.VMEM((nmem, *vector), f32),
                pltpu.VMEM((nmem, *vector), f32),
                pltpu.VMEM((4, nmem, *vector), f32),
                pltpu.VMEM((nmem * members, *vector), f32),
                pltpu.VMEM((4, *vector), f32),
                pltpu.VMEM((levels, *vector), f32),
                pltpu.VMEM((nmem, *vector), f32),
                pltpu.VMEM((levels, 5, *vector), f32),
                pltpu.VMEM((rows + 2 * REACH, 3, *vector), f32),
                pltpu.VMEM((nmem, *vector), f32),
                pltpu.VMEM((nmem, *vector), f32),
                pltpu.VMEM((nsx * nsy, *vector), f32),
                dma((2,)),
                dma((4,)),
                dma((2,)),
                dma((2,)),
                dma((2,)),
                dma((2,)),
                dma((2,)),
                dma((2,)),
                dma((1,)),
                dma((2,)),
                dma((2,)),
            ],
            compiler_params=pltpu.CompilerParams(collective_id=0, has_side_effects=True, vmem_limit_bytes=VMEM_GRANT),
            name="gather",
        )(child)
        count = 4.0 * 81.0 * (members * nmem - 1) * levels * rows * nsx * cols * nsy
        return pl.pallas_call(
            functools.partial(scale, count),
            out_shape=(
                jax.ShapeDtypeStruct((levels // nmem, rows, cols), f32),
                jax.ShapeDtypeStruct((levels, rows, cols), f32),
            ),
            in_specs=[vmem, vmem, vmem],
            out_specs=(vmem, vmem),
            compiler_params=pltpu.CompilerParams(vmem_limit_bytes=8 << 20),
            name="scale",
        )(z, total, means)

    return jax.shard_map(
        local,
        mesh=mesh,
        in_specs=(P("mem", None, "sx", "sy"),),
        out_specs=(P("mem", "sx", "sy"), P("mem", "sx", "sy")),
        check_vma=False,
    )
```

```python
import functools

import jax
import jax.numpy as jnp
import numpy as np
from jax import lax
from jax.experimental import pallas as pl
from jax.experimental.pallas import tpu as pltpu
from jax.sharding import PartitionSpec as P

MESH = pl.DeviceIdType.MESH
REACH = 4
LANES = 128
SUB = 8
VMEM_GRANT = 55_500_000


def gaspari_table(reach):
    offsets = np.arange(-reach, reach + 1) * 1.0
    dist = np.sqrt(offsets[:, None] ** 2 + offsets[None, :] ** 2) / 2.5
    near = -0.25 * dist**5 + 0.5 * dist**4 + 0.625 * dist**3 - 5.0 / 3.0 * dist**2 + 1.0
    safe = np.maximum(dist, 0.001)
    far = (
        dist**5 / 12.0
        - 0.5 * dist**4
        + 0.625 * dist**3
        + 5.0 / 3.0 * dist**2
        - 5.0 * dist
        + 4.0
        - 2.0 / (3.0 * safe)
    )
    table = np.where(dist <= 1.0, near, np.where(dist < 2.0, far, 0.0))
    return table / table.sum()


def gather(
    nmem,
    nsx,
    nsy,
    child_ref,
    z_ref,
    all_ref,
    means_ref,
    xbuf,
    pick,
    ybuf,
    psend,
    rbuf,
    pack,
    from_left,
    from_right,
    hsend,
    hbuf,
    abuf,
    sbuf,
    mbuf,
    mmsg,
    means,
    msg,
    q,
    odd,
    s1,
    s2,
    ld_sem,
    p1_sem,
    e_send,
    e_recv,
    h_sem,
    s1_sem,
    m_sem,
    q_sem,
    n_send,
    n_recv,
    s2_sem,
    known,
):
    members, levels, child_rows, child_cols = child_ref.shape
    rows = child_rows // 3
    half_rows = child_rows // 2
    mem = lax.axis_index("mem")
    sx = lax.axis_index("sx")
    sy = lax.axis_index("sy")
    total_members = members * nmem
    ring = nmem // 2
    z, y = mem // ring, lax.rem(mem, ring)

    def at(m=None, x=None, y=None):
        return {
            "mem": mem if m is None else m,
            "sx": sx if x is None else x,
            "sy": sy if y is None else y,
        }

    loads = []
    for half, owner_z in enumerate((1 - z, z)):
        first = pl.multiple_of(owner_z * half_rows, SUB)
        copy = pltpu.make_async_copy(
            child_ref.at[:, :, pl.ds(first, half_rows), :], xbuf.at[half], ld_sem.at[half]
        )
        copy.start()
        loads.append(copy)

    steps = [(1, 0), (1, 1), (1, 3), (1, 2), (0, 2), (0, 1), (0, 3)]
    spots = [lax.rem(y + b, ring) for _, b in steps]
    peers = [lax.rem(z + a, 2) * ring + spot for (a, _), spot in zip(steps, spots)]
    plane = [(a, b) for a in range(nsx) for b in range(nsy) if (a, b) != (0, 0)]
    plane_peers = [(lax.rem(sx + a, nsx), lax.rem(sy + b, nsy)) for a, b in plane]
    above, below = lax.rem(sx + 1, nsx), lax.rem(sx + nsx - 1, nsx)

    def send(src, dst, pair, device):
        copy = pltpu.make_async_remote_copy(
            src_ref=src,
            dst_ref=dst,
            send_sem=pair[0],
            recv_sem=pair[1],
            device_id=device,
            device_id_type=MESH,
        )
        copy.start()

    def settle(ref, sem, received):
        copy = pltpu.make_async_remote_copy(
            src_ref=ref,
            dst_ref=ref,
            send_sem=sem,
            recv_sem=sem,
            device_id=at(m=peers[0]),
            device_id_type=MESH,
        )
        if received:
            copy.wait_recv()
        else:
            copy.wait_send()

    def greet(sem, friend):
        pl.semaphore_signal(sem, inc=1, device_id=friend, device_id_type=MESH)

    def greet_around(sem):
        for a in (-1, 0, 1):
            for b in (-1, 0, 1):
                if (a, b) != (0, 0):
                    inside = (sx + a >= 0) & (sx + a < nsx) & (sy + b >= 0) & (sy + b < nsy)
                    friend = at(x=lax.rem(sx + a + nsx, nsx), y=lax.rem(sy + b + nsy, nsy))
                    pl.when(inside)(lambda: greet(sem, friend))

    tiles_x = 3 - jnp.where(sx == 0, 1, 0) - jnp.where(sx == nsx - 1, 1, 0)
    tiles_y = 3 - jnp.where(sy == 0, 1, 0) - jnp.where(sy == nsy - 1, 1, 0)
    around = tiles_x * tiles_y - 1
    barrier = pltpu.get_barrier_semaphore()
    for p in peers:
        greet(barrier, at(m=p))
    greet_around(barrier)

    zero = jnp.zeros((SUB, LANES), jnp.float32)

    width = 3 * LANES
    r_ids = lax.broadcasted_iota(jnp.int32, (width, LANES), 0)
    c_ids = lax.broadcasted_iota(jnp.int32, (width, LANES), 1)
    off = r_ids - 3 * c_ids
    pick[...] = jnp.where((off >= 0) & (off <= 2), 1.0, 0.0).astype(jnp.bfloat16)

    def post(first, count, n, sem):
        part = pl.ds(first, count)
        send(
            psend.at[1 - steps[n][0], spots[n], part],
            rbuf.at[n + 1, part],
            (p1_sem.at[0], p1_sem.at[sem]),
            at(m=peers[n]),
        )

    within = zero
    for half, owner_z in enumerate((1 - z, z)):
        loads[half].wait()
        for c in range(2):
            ybuf[c] = jnp.dot(
                xbuf[half, :, :, :, pl.ds(c * width, width)].reshape(-1, width),
                pick[...],
                preferred_element_type=jnp.float32,
            )
        for i in range(rows // 2):
            for c in range(2):
                p = []
                for m in range(members):
                    total = None
                    for a in range(3):
                        start = m * levels * half_rows + 3 * i + a
                        line = ybuf[c, pl.ds(start, levels, stride=half_rows), :]
                        total = line if total is None else total + line
                    p.append(total)
                up, down = p[0] + p[1], p[2] + p[3]
                left, right = p[0] - p[1], p[2] - p[3]
                owner, inside = i % ring, i // ring
                i2 = inside + owner_z - 2 * inside * owner_z
                psend[half, owner, 2 * i2 + c] = up + down
                for j, value in enumerate((up - down, left + right, left - right)):
                    psend[half, owner, 4 + 6 * i2 + 2 * j + c] = value
                    within += value * value
    def clear_rows(first):
        for row in range(first, first + REACH):
            for v in range(3):
                q[row, v] = zero

    def clear_side(ref):
        for d in range(nmem):
            ref[d] = zero

    pl.when(sx == 0)(lambda: clear_rows(0))
    pl.when(sx == nsx - 1)(lambda: clear_rows(REACH + rows))
    pl.when(sy == 0)(lambda: clear_side(from_left))
    pl.when(sy == nsy - 1)(lambda: clear_side(from_right))

    lane = lax.broadcasted_iota(jnp.int32, (SUB, LANES), 1)
    for d in range(nmem):
        half, owner = d // ring, d % ring
        packed = zero
        for j in range(members):
            for i2 in range(2):
                shift = 8 * j + 64 * i2
                k = 2 * i2 if j == 0 else 2 + 6 * i2 + 2 * j
                both = jnp.where(
                    lane < LANES // 2, psend[half, owner, k], psend[half, owner, k + 1]
                )
                if shift:
                    both = pltpu.roll(both, shift, 1)
                mine = ((lane - shift + 4 + LANES) & (LANES - 1)) < 8
                packed = jnp.where(mine, both, packed)
        pack[d] = packed

    pl.semaphore_wait(barrier, len(peers) + around)
    greet_around(known.at[0])
    for n in (3, 1, 2, 4, 0, 5, 6):
        post(0, 4, n, 1)

    @pl.when(sy < nsy - 1)
    def _():
        send(pack, from_left, (e_send.at[0], e_recv.at[0]), at(y=lax.rem(sy + 1, nsy)))

    @pl.when(sy > 0)
    def _():
        send(pack, from_right, (e_send.at[1], e_recv.at[1]), at(y=lax.rem(sy + nsy - 1, nsy)))

    for n in range(nmem - 1):
        post(4, 6, n, 2)
    for n in range(0):
        post(10, 6, n, 3)
    for k in range(16):
        rbuf[0, k] = psend[1, y, k]

    pl.when(sy > 0)(lambda: settle(from_left, e_recv.at[0], True))
    pl.when(sy < nsy - 1)(lambda: settle(from_right, e_recv.at[1], True))
    for d in range(nmem):
        hsend[d] = jnp.where((lane & 4) == 0, from_right[d], from_left[d])
    for n, (p, spot) in enumerate(zip(peers, spots)):
        send(
            hsend.at[(1 - steps[n][0]) * ring + spot],
            hbuf.at[n + 1],
            (h_sem.at[0], h_sem.at[1]),
            at(m=p),
        )
    hbuf[0] = hsend[ring + y]

    pl.semaphore_wait(known.at[0], around)
    greet_around(known.at[1])

    settle(rbuf.at[pl.ds(1, nmem - 1), pl.ds(0, 4)], p1_sem.at[1], True)
    var = within
    for v in range(4):
        total = rbuf[0, v]
        for o in range(1, nmem):
            total += rbuf[o, v]
        mbuf[v] = total * (1.0 / (9.0 * total_members))
        middle = total * (1.0 / nmem)
        for o in range(nmem):
            anom = rbuf[o, v] - middle
            abuf[v, o] = anom
            var += anom * anom
    s1[0] = jnp.sum(var, axis=0, keepdims=True)
    for n, p in enumerate(peers):
        send(s1.at[0], s1.at[n + 1], (s1_sem.at[0], s1_sem.at[1]), at(m=p))
    for n in range(nmem - 1):
        post(10, 6, n, 3)
    for l in range(levels):
        mmsg[l] = zero
        for v in range(4):
            mmsg[l, pl.ds(v, 1), :] = mbuf[v, pl.ds(l, 1), :]
    for p in peers:
        send(mmsg.at[p], means.at[mem], (m_sem.at[0], m_sem.at[1]), at(m=p))
    means[mem] = mmsg[mem]

    factor = 1.0 / (4.0 * 81.0 * (total_members - 1))

    def covariances(v, vectors):
        acc = [zero] * levels
        for ref, index in vectors:
            anom = ref[index]
            for l in range(levels):
                acc[l] += anom * ref[(*index, pl.ds(l, 1), slice(None))]
        for l in range(levels):
            msg[l, v] = acc[l] * factor

    def cells_of_row(i2, first):
        def column(c, carry):
            vectors = []
            for o in range(nmem):
                vectors.append((abuf, (2 * i2 + c, o)))
                vectors += [(rbuf, (o, 4 + 6 * i2 + 2 * j + c)) for j in range(members - 1)]
            covariances(first + c, vectors)
            return carry

        lax.fori_loop(0, 2, column, 0)

    settle(rbuf.at[pl.ds(1, nmem - 1), pl.ds(4, 6)], p1_sem.at[2], True)
    cells_of_row(0, 0)
    settle(hbuf.at[pl.ds(1, nmem - 1)], h_sem.at[1], True)
    total = hbuf[0]
    for o in range(1, nmem):
        total += hbuf[o]
    middle = total * (1.0 / nmem)
    for o in range(nmem):
        sbuf[members * o] = hbuf[o] - middle
        for j in range(1, members):
            sbuf[members * o + j] = pltpu.roll(hbuf[o], LANES - 8 * j, 1)
    covariances(2, [(sbuf, (t,)) for t in range(total_members)])

    edge_row = mem + z * (rows - nmem)
    sends_down = (z == 0) & (sx > 0)
    sends_up = (z == 1) & (sx < nsx - 1)
    edge_part, inner_part = pl.ds(0, 3), pl.ds(3, 2)

    @pl.when(sends_down)
    def _():
        for l in range(levels):
            pair = (n_send.at[0], n_recv.at[1])
            row = REACH + rows + mem
            send(msg.at[l, edge_part], q.at[row], pair, at(m=l, x=below))

    @pl.when(sends_up)
    def _():
        for l in range(levels):
            pair = (n_send.at[0], n_recv.at[0])
            row = mem - ring
            send(msg.at[l, edge_part], q.at[row], pair, at(m=l, x=above))

    for p in peers:
        pair = (q_sem.at[0], q_sem.at[1])
        send(msg.at[p, edge_part], q.at[REACH + edge_row], pair, at(m=p))
    for v in range(3):
        q[REACH + edge_row, v] = msg[mem, v]

    settle(s1.at[pl.ds(1, nmem - 1)], s1_sem.at[1], True)
    pl.semaphore_wait(known.at[1], around)
    s2[0] = jnp.sum(s1[...], axis=0)
    for n, (a, b) in enumerate(plane_peers):
        send(s2.at[0], s2.at[n + 1], (s2_sem.at[0], s2_sem.at[1]), at(x=a, y=b))

    settle(rbuf.at[pl.ds(1, nmem - 1), pl.ds(10, 6)], p1_sem.at[3], True)
    cells_of_row(1, 3)
    inner_row = REACH + mem
    for p in peers:
        pair = (q_sem.at[0], q_sem.at[1])
        send(msg.at[p, inner_part], q.at[REACH + inner_row, pl.ds(0, 2)], pair, at(m=p))
    for v in range(2):
        q[REACH + inner_row, v] = msg[mem, 3 + v]

    settle(means.at[pl.ds(0, nmem - 1)], m_sem.at[1], True)
    for d in range(nmem):
        means_ref[d] = means[d]
    settle(msg.at[pl.ds(0, nmem - 1)], q_sem.at[1], True)
    pl.when(sx > 0)(lambda: settle(q.at[pl.ds(0, REACH)], n_recv.at[0], True))
    pl.when(sx < nsx - 1)(lambda: settle(q.at[pl.ds(REACH + rows, REACH)], n_recv.at[1], True))

    table = gaspari_table(REACH)
    for d in range(nmem):
        row = d if d < ring else d + rows - nmem
        odd[d] = pltpu.roll(q[REACH + row, 2], LANES // 2, 1)

    def cells(row):
        inner = row - 2 * REACH
        side = odd[inner] if 0 <= inner < nmem else q[row, 2]
        return jnp.concatenate([q[row, 0], q[row, 1], side], axis=1)

    for i in range(rows):
        center = i + REACH
        lines = [cells(center)]
        for e in range(1, REACH + 1):
            lines.append(cells(center - e) + cells(center + e))
        out = None
        for f in range(REACH + 1):
            line = None
            for e in range(REACH + 1):
                weight = float(table[REACH + e, REACH + f])
                if weight != 0.0:
                    term = weight * lines[e]
                    line = term if line is None else line + term
            if f == 0:
                out = line
            else:
                out = out + pltpu.roll(line, f, 1) + pltpu.roll(line, width - f, 1)
        for c in range(2):
            z_ref[c, pl.ds(i, levels, stride=rows), :] = out[:, c * LANES : (c + 1) * LANES]

    settle(s2.at[pl.ds(1, len(plane))], s2_sem.at[1], True)
    all_ref[...] = jnp.sum(s2[...], axis=0)

    settle(rbuf.at[pl.ds(1, nmem - 1)], p1_sem.at[0], False)
    pl.when(sy < nsy - 1)(lambda: settle(pack, e_send.at[0], False))
    pl.when(sy > 0)(lambda: settle(pack, e_send.at[1], False))
    settle(hsend.at[pl.ds(0, nmem - 1)], h_sem.at[0], False)
    settle(s1.at[pl.ds(0, nmem - 1)], s1_sem.at[0], False)
    settle(mmsg.at[pl.ds(0, nmem - 1)], m_sem.at[0], False)
    settle(msg.at[pl.ds(0, nmem - 1)], q_sem.at[0], False)
    pl.when(sends_down | sends_up)(lambda: settle(q.at[pl.ds(0, levels)], n_send.at[0], False))
    settle(s2.at[pl.ds(0, len(plane))], s2_sem.at[0], False)


def scale(count, z_ref, all_ref, means_ref, mean_ref, cov_ref):
    levels, rows, cols = cov_ref.shape
    spread = jnp.sum(all_ref[...], keepdims=True) * (1.0 / count)
    inverse = 1.0 / (spread + 1e-6)
    for k in range(levels):
        for c in range(cols // LANES):
            block = z_ref[c, pl.ds(k * rows, rows), :]
            cov_ref[k, :, pl.ds(c * LANES, LANES)] = block * inverse
    for i in range(rows):
        inner = 1 if REACH <= i < rows - REACH else 0
        source = i - REACH if inner else i % (rows - 2 * REACH)
        for c in range(cols // LANES):
            row = means_ref[source, pl.ds(2 * inner + c, 1), :]
            mean_ref[0, pl.ds(i, 1), pl.ds(c * LANES, LANES)] = row


def solution(mesh):
    nmem, nsx, nsy = (mesh.shape[name] for name in ("mem", "sx", "sy"))

    def local(child):
        members, levels, child_rows, child_cols = child.shape
        rows, cols = child_rows // 3, child_cols // 3
        f32 = jnp.float32
        dma = pltpu.SemaphoreType.DMA
        vmem = pl.BlockSpec(memory_space=pltpu.VMEM)
        vector = (SUB, LANES)
        z, total, means = pl.pallas_call(
            functools.partial(gather, nmem, nsx, nsy),
            out_shape=(
                jax.ShapeDtypeStruct((2, levels * rows, LANES), f32),
                jax.ShapeDtypeStruct((1, LANES), f32),
                jax.ShapeDtypeStruct((nmem, *vector), f32),
            ),
            in_specs=[pl.BlockSpec(memory_space=pltpu.MemorySpace.HBM)],
            out_specs=(vmem, vmem, vmem),
            scratch_shapes=[
                pltpu.VMEM((2, members, levels, child_rows // 2, child_cols), child.dtype),
                pltpu.VMEM((3 * LANES, LANES), child.dtype),
                pltpu.VMEM((2, members * levels * child_rows // 2, LANES), f32),
                pltpu.VMEM((2, nmem // 2, 16, *vector), f32),
                pltpu.VMEM((nmem, 16, *vector), f32),
                pltpu.VMEM((nmem, *vector), f32),
                pltpu.VMEM((nmem, *vector), f32),
                pltpu.VMEM((nmem, *vector), f32),
                pltpu.VMEM((nmem, *vector), f32),
                pltpu.VMEM((nmem, *vector), f32),
                pltpu.VMEM((4, nmem, *vector), f32),
                pltpu.VMEM((nmem * members, *vector), f32),
                pltpu.VMEM((4, *vector), f32),
                pltpu.VMEM((levels, *vector), f32),
                pltpu.VMEM((nmem, *vector), f32),
                pltpu.VMEM((levels, 5, *vector), f32),
                pltpu.VMEM((rows + 2 * REACH, 3, *vector), f32),
                pltpu.VMEM((nmem, *vector), f32),
                pltpu.VMEM((nmem, 1, LANES), f32),
                pltpu.VMEM((nsx * nsy, 1, LANES), f32),
                dma((2,)),
                dma((4,)),
                dma((2,)),
                dma((2,)),
                dma((2,)),
                dma((2,)),
                dma((2,)),
                dma((2,)),
                dma((1,)),
                dma((2,)),
                dma((2,)),
                pltpu.SemaphoreType.REGULAR((2,)),
            ],
            compiler_params=pltpu.CompilerParams(collective_id=0, has_side_effects=True, vmem_limit_bytes=VMEM_GRANT),
            name="gather",
        )(child)
        count = 4.0 * 81.0 * (members * nmem - 1) * levels * rows * nsx * cols * nsy
        return pl.pallas_call(
            functools.partial(scale, count),
            out_shape=(
                jax.ShapeDtypeStruct((levels // nmem, rows, cols), f32),
                jax.ShapeDtypeStruct((levels, rows, cols), f32),
            ),
            in_specs=[vmem, vmem, vmem],
            out_specs=(vmem, vmem),
            compiler_params=pltpu.CompilerParams(vmem_limit_bytes=8 << 20),
            name="scale",
        )(z, total, means)

    return jax.shard_map(
        local,
        mesh=mesh,
        in_specs=(P("mem", None, "sx", "sy"),),
        out_specs=(P("mem", "sx", "sy"), P("mem", "sx", "sy")),
        check_vma=False,
    )
```

```python
import functools

import jax
import jax.numpy as jnp
import numpy as np
from jax import lax
from jax.experimental import pallas as pl
from jax.experimental.pallas import tpu as pltpu
from jax.sharding import PartitionSpec as P

MESH = pl.DeviceIdType.MESH
REACH = 4
LANES = 128
SUB = 8
VMEM_GRANT = 55_500_000


def gaspari_table(reach):
    offsets = np.arange(-reach, reach + 1) * 1.0
    dist = np.sqrt(offsets[:, None] ** 2 + offsets[None, :] ** 2) / 2.5
    near = -0.25 * dist**5 + 0.5 * dist**4 + 0.625 * dist**3 - 5.0 / 3.0 * dist**2 + 1.0
    safe = np.maximum(dist, 0.001)
    far = (
        dist**5 / 12.0
        - 0.5 * dist**4
        + 0.625 * dist**3
        + 5.0 / 3.0 * dist**2
        - 5.0 * dist
        + 4.0
        - 2.0 / (3.0 * safe)
    )
    table = np.where(dist <= 1.0, near, np.where(dist < 2.0, far, 0.0))
    return table / table.sum()


def gather(
    nmem,
    nsx,
    nsy,
    child_ref,
    z_ref,
    all_ref,
    means_ref,
    xbuf,
    pick,
    ybuf,
    psend,
    rbuf,
    pack,
    from_left,
    from_right,
    hsend,
    hbuf,
    abuf,
    sbuf,
    mbuf,
    mmsg,
    means,
    msg,
    q,
    odd,
    s1,
    s2,
    ld_sem,
    p1_sem,
    e_send,
    e_recv,
    h_sem,
    s1_sem,
    m_sem,
    q_sem,
    n_send,
    n_recv,
    s2_sem,
    known,
):
    members, levels, child_rows, child_cols = child_ref.shape
    rows = child_rows // 3
    half_rows = child_rows // 2
    mem = lax.axis_index("mem")
    sx = lax.axis_index("sx")
    sy = lax.axis_index("sy")
    total_members = members * nmem
    ring = nmem // 2
    z, y = mem // ring, lax.rem(mem, ring)

    def at(m=None, x=None, y=None):
        return {
            "mem": mem if m is None else m,
            "sx": sx if x is None else x,
            "sy": sy if y is None else y,
        }

    loads = []
    for half, owner_z in enumerate((1 - z, z)):
        first = pl.multiple_of(owner_z * half_rows, SUB)
        copy = pltpu.make_async_copy(
            child_ref.at[:, :, pl.ds(first, half_rows), :], xbuf.at[half], ld_sem.at[half]
        )
        copy.start()
        loads.append(copy)

    steps = [(1, 0), (1, 1), (1, 3), (1, 2), (0, 2), (0, 1), (0, 3)]
    spots = [lax.rem(y + b, ring) for _, b in steps]
    peers = [lax.rem(z + a, 2) * ring + spot for (a, _), spot in zip(steps, spots)]
    plane = [(a, b) for a in range(nsx) for b in range(nsy) if (a, b) != (0, 0)]
    plane_peers = [(lax.rem(sx + a, nsx), lax.rem(sy + b, nsy)) for a, b in plane]
    above, below = lax.rem(sx + 1, nsx), lax.rem(sx + nsx - 1, nsx)

    def send(src, dst, pair, device):
        copy = pltpu.make_async_remote_copy(
            src_ref=src,
            dst_ref=dst,
            send_sem=pair[0],
            recv_sem=pair[1],
            device_id=device,
            device_id_type=MESH,
        )
        copy.start()

    def settle(ref, sem, received):
        copy = pltpu.make_async_remote_copy(
            src_ref=ref,
            dst_ref=ref,
            send_sem=sem,
            recv_sem=sem,
            device_id=at(m=peers[0]),
            device_id_type=MESH,
        )
        if received:
            copy.wait_recv()
        else:
            copy.wait_send()

    def greet(sem, friend):
        pl.semaphore_signal(sem, inc=1, device_id=friend, device_id_type=MESH)

    fellows = (mem, peers[0])

    def greet_around(sem, whom):
        for a in (-1, 0, 1):
            for b in (-1, 0, 1):
                if (a, b) != (0, 0):
                    inside = (sx + a >= 0) & (sx + a < nsx) & (sy + b >= 0) & (sy + b < nsy)
                    x, y2 = lax.rem(sx + a + nsx, nsx), lax.rem(sy + b + nsy, nsy)

                    @pl.when(inside)
                    def _():
                        for m in whom:
                            greet(sem, at(m=m, x=x, y=y2))

    tiles_x = 3 - jnp.where(sx == 0, 1, 0) - jnp.where(sx == nsx - 1, 1, 0)
    tiles_y = 3 - jnp.where(sy == 0, 1, 0) - jnp.where(sy == nsy - 1, 1, 0)
    around = tiles_x * tiles_y - 1
    barrier = pltpu.get_barrier_semaphore()
    for p in peers:
        greet(barrier, at(m=p))
    greet_around(barrier, fellows)

    zero = jnp.zeros((SUB, LANES), jnp.float32)

    width = 3 * LANES
    r_ids = lax.broadcasted_iota(jnp.int32, (width, LANES), 0)
    c_ids = lax.broadcasted_iota(jnp.int32, (width, LANES), 1)
    off = r_ids - 3 * c_ids
    pick[...] = jnp.where((off >= 0) & (off <= 2), 1.0, 0.0).astype(jnp.bfloat16)

    def post(first, count, n, sem):
        part = pl.ds(first, count)
        send(
            psend.at[1 - steps[n][0], spots[n], part],
            rbuf.at[n + 1, part],
            (p1_sem.at[0], p1_sem.at[sem]),
            at(m=peers[n]),
        )

    within = zero
    for half, owner_z in enumerate((1 - z, z)):
        loads[half].wait()
        for c in range(2):
            ybuf[c] = jnp.dot(
                xbuf[half, :, :, :, pl.ds(c * width, width)].reshape(-1, width),
                pick[...],
                preferred_element_type=jnp.float32,
            )
        for i in range(rows // 2):
            for c in range(2):
                p = []
                for m in range(members):
                    total = None
                    for a in range(3):
                        start = m * levels * half_rows + 3 * i + a
                        line = ybuf[c, pl.ds(start, levels, stride=half_rows), :]
                        total = line if total is None else total + line
                    p.append(total)
                up, down = p[0] + p[1], p[2] + p[3]
                left, right = p[0] - p[1], p[2] - p[3]
                owner, inside = i % ring, i // ring
                i2 = inside + owner_z - 2 * inside * owner_z
                psend[half, owner, 2 * i2 + c] = up + down
                for j, value in enumerate((up - down, left + right, left - right)):
                    psend[half, owner, 4 + 6 * i2 + 2 * j + c] = value
                    within += value * value
    pl.semaphore_wait(barrier, len(peers) + 2 * around)
    greet_around(known.at[0], (mem,))
    for n in (3, 1, 2, 4, 0, 5, 6):
        post(0, 4, n, 1)

    def clear_rows(first):
        for row in range(first, first + REACH):
            for v in range(3):
                q[row, v] = zero

    def clear_side(ref):
        for d in range(nmem):
            ref[d] = zero

    pl.when(sx == 0)(lambda: clear_rows(0))
    pl.when(sx == nsx - 1)(lambda: clear_rows(REACH + rows))
    pl.when(sy == 0)(lambda: clear_side(from_left))
    pl.when(sy == nsy - 1)(lambda: clear_side(from_right))

    lane = lax.broadcasted_iota(jnp.int32, (SUB, LANES), 1)
    for d in range(nmem):
        half, owner = d // ring, d % ring
        packed = zero
        for j in range(members):
            for i2 in range(2):
                shift = 8 * j + 64 * i2
                k = 2 * i2 if j == 0 else 2 + 6 * i2 + 2 * j
                both = jnp.where(
                    lane < LANES // 2, psend[half, owner, k], psend[half, owner, k + 1]
                )
                if shift:
                    both = pltpu.roll(both, shift, 1)
                mine = ((lane - shift + 4 + LANES) & (LANES - 1)) < 8
                packed = jnp.where(mine, both, packed)
        pack[d] = packed

    @pl.when(sy < nsy - 1)
    def _():
        send(pack, from_left, (e_send.at[0], e_recv.at[0]), at(y=lax.rem(sy + 1, nsy)))

    @pl.when(sy > 0)
    def _():
        send(pack, from_right, (e_send.at[1], e_recv.at[1]), at(y=lax.rem(sy + nsy - 1, nsy)))

    for n in range(nmem - 1):
        post(4, 6, n, 2)
    for n in range(0):
        post(10, 6, n, 3)
    for k in range(16):
        rbuf[0, k] = psend[1, y, k]

    pl.when(sy > 0)(lambda: settle(from_left, e_recv.at[0], True))
    pl.when(sy < nsy - 1)(lambda: settle(from_right, e_recv.at[1], True))
    for d in range(nmem):
        hsend[d] = jnp.where((lane & 4) == 0, from_right[d], from_left[d])
    for n, (p, spot) in enumerate(zip(peers, spots)):
        send(
            hsend.at[(1 - steps[n][0]) * ring + spot],
            hbuf.at[n + 1],
            (h_sem.at[0], h_sem.at[1]),
            at(m=p),
        )
    hbuf[0] = hsend[ring + y]

    pl.semaphore_wait(known.at[0], around)
    greet_around(known.at[1], (mem,))

    settle(rbuf.at[pl.ds(1, nmem - 1), pl.ds(0, 4)], p1_sem.at[1], True)
    var = within
    for v in range(4):
        total = rbuf[0, v]
        for o in range(1, nmem):
            total += rbuf[o, v]
        mbuf[v] = total * (1.0 / (9.0 * total_members))
        middle = total * (1.0 / nmem)
        for o in range(nmem):
            anom = rbuf[o, v] - middle
            abuf[v, o] = anom
            var += anom * anom
    s1[0] = jnp.sum(var, axis=0, keepdims=True)
    for n, p in enumerate(peers[ring:]):
        send(s1.at[0], s1.at[n + 1], (s1_sem.at[0], s1_sem.at[1]), at(m=p))
    for n in range(nmem - 1):
        post(10, 6, n, 3)
    for l in range(levels):
        mmsg[l] = zero
        for v in range(4):
            mmsg[l, pl.ds(v, 1), :] = mbuf[v, pl.ds(l, 1), :]
    for p in peers:
        send(mmsg.at[p], means.at[mem], (m_sem.at[0], m_sem.at[1]), at(m=p))
    means[mem] = mmsg[mem]

    factor = 1.0 / (4.0 * 81.0 * (total_members - 1))

    def covariances(v, vectors):
        acc = [zero] * levels
        for ref, index in vectors:
            anom = ref[index]
            for l in range(levels):
                acc[l] += anom * ref[(*index, pl.ds(l, 1), slice(None))]
        for l in range(levels):
            msg[l, v] = acc[l] * factor

    def cells_of_row(i2, first):
        def column(c, carry):
            vectors = []
            for o in range(nmem):
                vectors.append((abuf, (2 * i2 + c, o)))
                vectors += [(rbuf, (o, 4 + 6 * i2 + 2 * j + c)) for j in range(members - 1)]
            covariances(first + c, vectors)
            return carry

        lax.fori_loop(0, 2, column, 0)

    settle(rbuf.at[pl.ds(1, nmem - 1), pl.ds(4, 6)], p1_sem.at[2], True)
    cells_of_row(0, 0)
    settle(hbuf.at[pl.ds(1, nmem - 1)], h_sem.at[1], True)
    total = hbuf[0]
    for o in range(1, nmem):
        total += hbuf[o]
    middle = total * (1.0 / nmem)
    for o in range(nmem):
        sbuf[members * o] = hbuf[o] - middle
        for j in range(1, members):
            sbuf[members * o + j] = pltpu.roll(hbuf[o], LANES - 8 * j, 1)
    covariances(2, [(sbuf, (t,)) for t in range(total_members)])

    edge_row = mem + z * (rows - nmem)
    sends_down = (z == 0) & (sx > 0)
    sends_up = (z == 1) & (sx < nsx - 1)
    edge_part, inner_part = pl.ds(0, 3), pl.ds(3, 2)

    @pl.when(sends_down)
    def _():
        for l in range(levels):
            pair = (n_send.at[0], n_recv.at[1])
            row = REACH + rows + mem
            send(msg.at[l, edge_part], q.at[row], pair, at(m=l, x=below))

    @pl.when(sends_up)
    def _():
        for l in range(levels):
            pair = (n_send.at[0], n_recv.at[0])
            row = mem - ring
            send(msg.at[l, edge_part], q.at[row], pair, at(m=l, x=above))

    for p in peers:
        pair = (q_sem.at[0], q_sem.at[1])
        send(msg.at[p, edge_part], q.at[REACH + edge_row], pair, at(m=p))
    for v in range(3):
        q[REACH + edge_row, v] = msg[mem, v]

    settle(s1.at[pl.ds(1, ring - 1)], s1_sem.at[1], True)
    pl.semaphore_wait(known.at[1], around)
    s2[0] = jnp.sum(s1[...], axis=0)
    others = [(m, a, b) for a, b in plane_peers for m in fellows] + [(peers[0], sx, sy)]
    for n, (m, a, b) in enumerate(others):
        send(s2.at[0], s2.at[n + 1], (s2_sem.at[0], s2_sem.at[1]), at(m, a, b))

    settle(rbuf.at[pl.ds(1, nmem - 1), pl.ds(10, 6)], p1_sem.at[3], True)
    cells_of_row(1, 3)
    inner_row = REACH + mem
    for p in peers:
        pair = (q_sem.at[0], q_sem.at[1])
        send(msg.at[p, inner_part], q.at[REACH + inner_row, pl.ds(0, 2)], pair, at(m=p))
    for v in range(2):
        q[REACH + inner_row, v] = msg[mem, 3 + v]

    settle(means.at[pl.ds(0, nmem - 1)], m_sem.at[1], True)
    for d in range(nmem):
        means_ref[d] = means[d]
    settle(msg.at[pl.ds(0, nmem - 1)], q_sem.at[1], True)
    pl.when(sx > 0)(lambda: settle(q.at[pl.ds(0, REACH)], n_recv.at[0], True))
    pl.when(sx < nsx - 1)(lambda: settle(q.at[pl.ds(REACH + rows, REACH)], n_recv.at[1], True))

    table = gaspari_table(REACH)
    for d in range(nmem):
        row = d if d < ring else d + rows - nmem
        odd[d] = pltpu.roll(q[REACH + row, 2], LANES // 2, 1)

    def cells(row):
        inner = row - 2 * REACH
        side = odd[inner] if 0 <= inner < nmem else q[row, 2]
        return jnp.concatenate([q[row, 0], q[row, 1], side], axis=1)

    for i in range(rows):
        center = i + REACH
        lines = [cells(center)]
        for e in range(1, REACH + 1):
            lines.append(cells(center - e) + cells(center + e))
        out = None
        for f in range(REACH + 1):
            line = None
            for e in range(REACH + 1):
                weight = float(table[REACH + e, REACH + f])
                if weight != 0.0:
                    term = weight * lines[e]
                    line = term if line is None else line + term
            if f == 0:
                out = line
            else:
                out = out + pltpu.roll(line, f, 1) + pltpu.roll(line, width - f, 1)
        for c in range(2):
            z_ref[c, pl.ds(i, levels, stride=rows), :] = out[:, c * LANES : (c + 1) * LANES]

    settle(s2.at[pl.ds(1, len(others))], s2_sem.at[1], True)
    all_ref[...] = jnp.sum(s2[...], axis=0)

    settle(rbuf.at[pl.ds(1, nmem - 1)], p1_sem.at[0], False)
    pl.when(sy < nsy - 1)(lambda: settle(pack, e_send.at[0], False))
    pl.when(sy > 0)(lambda: settle(pack, e_send.at[1], False))
    settle(hsend.at[pl.ds(0, nmem - 1)], h_sem.at[0], False)
    settle(s1.at[pl.ds(1, ring - 1)], s1_sem.at[0], False)
    settle(mmsg.at[pl.ds(0, nmem - 1)], m_sem.at[0], False)
    settle(msg.at[pl.ds(0, nmem - 1)], q_sem.at[0], False)
    pl.when(sends_down | sends_up)(lambda: settle(q.at[pl.ds(0, levels)], n_send.at[0], False))
    settle(s2.at[pl.ds(1, len(others))], s2_sem.at[0], False)


def scale(count, z_ref, all_ref, means_ref, mean_ref, cov_ref):
    levels, rows, cols = cov_ref.shape
    spread = jnp.sum(all_ref[...], keepdims=True) * (1.0 / count)
    inverse = 1.0 / (spread + 1e-6)
    for k in range(levels):
        for c in range(cols // LANES):
            block = z_ref[c, pl.ds(k * rows, rows), :]
            cov_ref[k, :, pl.ds(c * LANES, LANES)] = block * inverse
    for i in range(rows):
        inner = 1 if REACH <= i < rows - REACH else 0
        source = i - REACH if inner else i % (rows - 2 * REACH)
        for c in range(cols // LANES):
            row = means_ref[source, pl.ds(2 * inner + c, 1), :]
            mean_ref[0, pl.ds(i, 1), pl.ds(c * LANES, LANES)] = row


def solution(mesh):
    nmem, nsx, nsy = (mesh.shape[name] for name in ("mem", "sx", "sy"))

    def local(child):
        members, levels, child_rows, child_cols = child.shape
        rows, cols = child_rows // 3, child_cols // 3
        f32 = jnp.float32
        dma = pltpu.SemaphoreType.DMA
        vmem = pl.BlockSpec(memory_space=pltpu.VMEM)
        vector = (SUB, LANES)
        z, total, means = pl.pallas_call(
            functools.partial(gather, nmem, nsx, nsy),
            out_shape=(
                jax.ShapeDtypeStruct((2, levels * rows, LANES), f32),
                jax.ShapeDtypeStruct((1, LANES), f32),
                jax.ShapeDtypeStruct((nmem, *vector), f32),
            ),
            in_specs=[pl.BlockSpec(memory_space=pltpu.MemorySpace.HBM)],
            out_specs=(vmem, vmem, vmem),
            scratch_shapes=[
                pltpu.VMEM((2, members, levels, child_rows // 2, child_cols), child.dtype),
                pltpu.VMEM((3 * LANES, LANES), child.dtype),
                pltpu.VMEM((2, members * levels * child_rows // 2, LANES), f32),
                pltpu.VMEM((2, nmem // 2, 16, *vector), f32),
                pltpu.VMEM((nmem, 16, *vector), f32),
                pltpu.VMEM((nmem, *vector), f32),
                pltpu.VMEM((nmem, *vector), f32),
                pltpu.VMEM((nmem, *vector), f32),
                pltpu.VMEM((nmem, *vector), f32),
                pltpu.VMEM((nmem, *vector), f32),
                pltpu.VMEM((4, nmem, *vector), f32),
                pltpu.VMEM((nmem * members, *vector), f32),
                pltpu.VMEM((4, *vector), f32),
                pltpu.VMEM((levels, *vector), f32),
                pltpu.VMEM((nmem, *vector), f32),
                pltpu.VMEM((levels, 5, *vector), f32),
                pltpu.VMEM((rows + 2 * REACH, 3, *vector), f32),
                pltpu.VMEM((nmem, *vector), f32),
                pltpu.VMEM((nmem // 2, 1, LANES), f32),
                pltpu.VMEM((2 * nsx * nsy, 1, LANES), f32),
                dma((2,)),
                dma((4,)),
                dma((2,)),
                dma((2,)),
                dma((2,)),
                dma((2,)),
                dma((2,)),
                dma((2,)),
                dma((1,)),
                dma((2,)),
                dma((2,)),
                pltpu.SemaphoreType.REGULAR((2,)),
            ],
            compiler_params=pltpu.CompilerParams(collective_id=0, has_side_effects=True, vmem_limit_bytes=VMEM_GRANT),
            name="gather",
        )(child)
        count = 4.0 * 81.0 * (members * nmem - 1) * levels * rows * nsx * cols * nsy
        return pl.pallas_call(
            functools.partial(scale, count),
            out_shape=(
                jax.ShapeDtypeStruct((levels // nmem, rows, cols), f32),
                jax.ShapeDtypeStruct((levels, rows, cols), f32),
            ),
            in_specs=[vmem, vmem, vmem],
            out_specs=(vmem, vmem),
            compiler_params=pltpu.CompilerParams(vmem_limit_bytes=8 << 20),
            name="scale",
        )(z, total, means)

    return jax.shard_map(
        local,
        mesh=mesh,
        in_specs=(P("mem", None, "sx", "sy"),),
        out_specs=(P("mem", "sx", "sy"), P("mem", "sx", "sy")),
        check_vma=False,
    )
```

```python
import functools

import jax
import jax.numpy as jnp
import numpy as np
from jax import lax
from jax.experimental import pallas as pl
from jax.experimental.pallas import tpu as pltpu
from jax.sharding import PartitionSpec as P

MESH = pl.DeviceIdType.MESH
REACH = 4
LANES = 128
SUB = 8
VMEM_GRANT = 55_500_000


def gaspari_table(reach):
    offsets = np.arange(-reach, reach + 1) * 1.0
    dist = np.sqrt(offsets[:, None] ** 2 + offsets[None, :] ** 2) / 2.5
    near = -0.25 * dist**5 + 0.5 * dist**4 + 0.625 * dist**3 - 5.0 / 3.0 * dist**2 + 1.0
    safe = np.maximum(dist, 0.001)
    far = (
        dist**5 / 12.0
        - 0.5 * dist**4
        + 0.625 * dist**3
        + 5.0 / 3.0 * dist**2
        - 5.0 * dist
        + 4.0
        - 2.0 / (3.0 * safe)
    )
    table = np.where(dist <= 1.0, near, np.where(dist < 2.0, far, 0.0))
    return table / table.sum()


def gather(
    nmem,
    nsx,
    nsy,
    child_ref,
    z_ref,
    all_ref,
    means_ref,
    xbuf,
    pick,
    ybuf,
    psend,
    rbuf,
    pack,
    from_left,
    from_right,
    hsend,
    hbuf,
    abuf,
    sbuf,
    mbuf,
    mmsg,
    means,
    msg,
    q,
    odd,
    s1,
    s2,
    ld_sem,
    p1_sem,
    e_send,
    e_recv,
    h_sem,
    s1_sem,
    m_sem,
    q_sem,
    n_send,
    n_recv,
    s2_sem,
    known,
):
    members, levels, child_rows, child_cols = child_ref.shape
    rows = child_rows // 3
    half_rows = child_rows // 2
    mem = lax.axis_index("mem")
    sx = lax.axis_index("sx")
    sy = lax.axis_index("sy")
    total_members = members * nmem
    ring = nmem // 2
    z, y = mem // ring, lax.rem(mem, ring)

    def at(m=None, x=None, y=None):
        return {
            "mem": mem if m is None else m,
            "sx": sx if x is None else x,
            "sy": sy if y is None else y,
        }

    loads = []
    for half, owner_z in enumerate((1 - z, z)):
        first = pl.multiple_of(owner_z * half_rows, SUB)
        copy = pltpu.make_async_copy(
            child_ref.at[:, :, pl.ds(first, half_rows), :], xbuf.at[half], ld_sem.at[half]
        )
        copy.start()
        loads.append(copy)

    steps = [(1, 0), (1, 1), (1, 3), (1, 2), (0, 2), (0, 1), (0, 3)]
    spots = [lax.rem(y + b, ring) for _, b in steps]
    peers = [lax.rem(z + a, 2) * ring + spot for (a, _), spot in zip(steps, spots)]
    plane = [(a, b) for a in range(nsx) for b in range(nsy) if (a, b) != (0, 0)]
    plane_peers = [(lax.rem(sx + a, nsx), lax.rem(sy + b, nsy)) for a, b in plane]
    above, below = lax.rem(sx + 1, nsx), lax.rem(sx + nsx - 1, nsx)

    def send(src, dst, pair, device):
        copy = pltpu.make_async_remote_copy(
            src_ref=src,
            dst_ref=dst,
            send_sem=pair[0],
            recv_sem=pair[1],
            device_id=device,
            device_id_type=MESH,
        )
        copy.start()

    def settle(ref, sem, received):
        copy = pltpu.make_async_remote_copy(
            src_ref=ref,
            dst_ref=ref,
            send_sem=sem,
            recv_sem=sem,
            device_id=at(m=peers[0]),
            device_id_type=MESH,
        )
        if received:
            copy.wait_recv()
        else:
            copy.wait_send()

    def greet(sem, friend):
        pl.semaphore_signal(sem, inc=1, device_id=friend, device_id_type=MESH)

    fellows = (mem, peers[0])

    def greet_around(sem, whom):
        for a in (-1, 0, 1):
            for b in (-1, 0, 1):
                if (a, b) != (0, 0):
                    inside = (sx + a >= 0) & (sx + a < nsx) & (sy + b >= 0) & (sy + b < nsy)
                    x, y2 = lax.rem(sx + a + nsx, nsx), lax.rem(sy + b + nsy, nsy)

                    @pl.when(inside)
                    def _():
                        for m in whom:
                            greet(sem, at(m=m, x=x, y=y2))

    tiles_x = 3 - jnp.where(sx == 0, 1, 0) - jnp.where(sx == nsx - 1, 1, 0)
    tiles_y = 3 - jnp.where(sy == 0, 1, 0) - jnp.where(sy == nsy - 1, 1, 0)
    around = tiles_x * tiles_y - 1
    barrier = pltpu.get_barrier_semaphore()
    for p in peers:
        greet(barrier, at(m=p))
    greet_around(barrier, fellows)

    zero = jnp.zeros((SUB, LANES), jnp.float32)

    width = 3 * LANES
    r_ids = lax.broadcasted_iota(jnp.int32, (width, LANES), 0)
    c_ids = lax.broadcasted_iota(jnp.int32, (width, LANES), 1)
    off = r_ids - 3 * c_ids
    pick[...] = jnp.where((off >= 0) & (off <= 2), 1.0, 0.0).astype(jnp.bfloat16)

    def post(first, count, n, sem):
        part = pl.ds(first, count)
        send(
            psend.at[1 - steps[n][0], spots[n], part],
            rbuf.at[n + 1, part],
            (p1_sem.at[0], p1_sem.at[sem]),
            at(m=peers[n]),
        )

    within = zero
    for half, owner_z in enumerate((1 - z, z)):
        loads[half].wait()
        for c in range(2):
            ybuf[c] = jnp.dot(
                xbuf[half, :, :, :, pl.ds(c * width, width)].reshape(-1, width),
                pick[...],
                preferred_element_type=jnp.float32,
            )
        for i in range(rows // 2):
            for c in range(2):
                p = []
                for m in range(members):
                    total = None
                    for a in range(3):
                        start = m * levels * half_rows + 3 * i + a
                        line = ybuf[c, pl.ds(start, levels, stride=half_rows), :]
                        total = line if total is None else total + line
                    p.append(total)
                up, down = p[0] + p[1], p[2] + p[3]
                left, right = p[0] - p[1], p[2] - p[3]
                owner, inside = i % ring, i // ring
                i2 = inside + owner_z - 2 * inside * owner_z
                psend[half, owner, 2 * i2 + c] = up + down
                for j, value in enumerate((up - down, left + right, left - right)):
                    psend[half, owner, 4 + 6 * i2 + 2 * j + c] = value
                    within += value * value
    pl.semaphore_wait(barrier, len(peers) + 2 * around)
    greet_around(known.at[0], (mem,))
    for n in (3, 1, 2, 4, 0, 5, 6):
        post(0, 4, n, 1)

    def clear_rows(first):
        for row in range(first, first + REACH):
            for v in range(3):
                q[row, v] = zero

    def clear_side(ref):
        for d in range(nmem):
            ref[d] = zero

    pl.when(sx == 0)(lambda: clear_rows(0))
    pl.when(sx == nsx - 1)(lambda: clear_rows(REACH + rows))
    pl.when(sy == 0)(lambda: clear_side(from_left))
    pl.when(sy == nsy - 1)(lambda: clear_side(from_right))

    lane = lax.broadcasted_iota(jnp.int32, (SUB, LANES), 1)
    for d in range(nmem):
        half, owner = d // ring, d % ring
        packed = zero
        for j in range(members):
            for i2 in range(2):
                shift = 8 * j + 64 * i2
                k = 2 * i2 if j == 0 else 2 + 6 * i2 + 2 * j
                both = jnp.where(
                    lane < LANES // 2, psend[half, owner, k], psend[half, owner, k + 1]
                )
                if shift:
                    both = pltpu.roll(both, shift, 1)
                mine = ((lane - shift + 4 + LANES) & (LANES - 1)) < 8
                packed = jnp.where(mine, both, packed)
        pack[d] = packed

    @pl.when(sy < nsy - 1)
    def _():
        send(pack, from_left, (e_send.at[0], e_recv.at[0]), at(y=lax.rem(sy + 1, nsy)))

    @pl.when(sy > 0)
    def _():
        send(pack, from_right, (e_send.at[1], e_recv.at[1]), at(y=lax.rem(sy + nsy - 1, nsy)))

    late = sy + 2 * (sx // 2) >= 4

    def post_edge_rows(some):
        for n in some:
            post(4, 6, n, 2)

    pl.when(~late)(lambda: post_edge_rows(range(nmem - 1)))
    for k in range(16):
        rbuf[0, k] = psend[1, y, k]

    pl.semaphore_wait(known.at[0], around)
    greet_around(known.at[1], (mem,))
    pl.when(late)(lambda: post_edge_rows(range(7)))

    pl.when(sy > 0)(lambda: settle(from_left, e_recv.at[0], True))
    pl.when(sy < nsy - 1)(lambda: settle(from_right, e_recv.at[1], True))
    for d in range(nmem):
        hsend[d] = jnp.where((lane & 4) == 0, from_right[d], from_left[d])

    def pass_edges():
        for n, (p, spot) in enumerate(zip(peers, spots)):
            owner = (1 - steps[n][0]) * ring + spot
            send(hsend.at[owner], hbuf.at[n + 1], (h_sem.at[0], h_sem.at[1]), at(m=p))

    pl.when(~late)(pass_edges)
    hbuf[0] = hsend[ring + y]

    settle(rbuf.at[pl.ds(1, nmem - 1), pl.ds(0, 4)], p1_sem.at[1], True)
    var = within
    for v in range(4):
        total = rbuf[0, v]
        for o in range(1, nmem):
            total += rbuf[o, v]
        mbuf[v] = total * (1.0 / (9.0 * total_members))
        middle = total * (1.0 / nmem)
        for o in range(nmem):
            anom = rbuf[o, v] - middle
            abuf[v, o] = anom
            var += anom * anom
    s1[0] = jnp.sum(var, axis=0, keepdims=True)
    for n, p in enumerate(peers[ring:]):
        send(s1.at[0], s1.at[n + 1], (s1_sem.at[0], s1_sem.at[1]), at(m=p))
    pl.when(late)(pass_edges)
    for n in range(nmem - 1):
        post(10, 6, n, 3)
    for l in range(levels):
        mmsg[l] = zero
        for v in range(4):
            mmsg[l, pl.ds(v, 1), :] = mbuf[v, pl.ds(l, 1), :]
    for p in peers:
        send(mmsg.at[p], means.at[mem], (m_sem.at[0], m_sem.at[1]), at(m=p))
    means[mem] = mmsg[mem]

    factor = 1.0 / (4.0 * 81.0 * (total_members - 1))

    def covariances(v, vectors):
        acc = [zero] * levels
        for ref, index in vectors:
            anom = ref[index]
            for l in range(levels):
                acc[l] += anom * ref[(*index, pl.ds(l, 1), slice(None))]
        for l in range(levels):
            msg[l, v] = acc[l] * factor

    def cells_of_row(i2, first):
        def column(c, carry):
            vectors = []
            for o in range(nmem):
                vectors.append((abuf, (2 * i2 + c, o)))
                vectors += [(rbuf, (o, 4 + 6 * i2 + 2 * j + c)) for j in range(members - 1)]
            covariances(first + c, vectors)
            return carry

        lax.fori_loop(0, 2, column, 0)

    others = [(m, a, b) for a, b in plane_peers for m in fellows] + [(peers[0], sx, sy)]

    def spread_on():
        settle(s1.at[pl.ds(1, ring - 1)], s1_sem.at[1], True)
        pl.semaphore_wait(known.at[1], around)
        s2[0] = jnp.sum(s1[...], axis=0)
        for n, (m, a, b) in enumerate(others):
            send(s2.at[0], s2.at[n + 1], (s2_sem.at[0], s2_sem.at[1]), at(m, a, b))

    pl.when(late)(spread_on)
    settle(rbuf.at[pl.ds(1, nmem - 1), pl.ds(4, 6)], p1_sem.at[2], True)
    cells_of_row(0, 0)
    settle(hbuf.at[pl.ds(1, nmem - 1)], h_sem.at[1], True)
    total = hbuf[0]
    for o in range(1, nmem):
        total += hbuf[o]
    middle = total * (1.0 / nmem)
    for o in range(nmem):
        sbuf[members * o] = hbuf[o] - middle
        for j in range(1, members):
            sbuf[members * o + j] = pltpu.roll(hbuf[o], LANES - 8 * j, 1)
    covariances(2, [(sbuf, (t,)) for t in range(total_members)])

    edge_row = mem + z * (rows - nmem)
    sends_down = (z == 0) & (sx > 0)
    sends_up = (z == 1) & (sx < nsx - 1)
    edge_part, inner_part = pl.ds(0, 3), pl.ds(3, 2)

    @pl.when(sends_down)
    def _():
        for l in range(levels):
            pair = (n_send.at[0], n_recv.at[1])
            row = REACH + rows + mem
            send(msg.at[l, edge_part], q.at[row], pair, at(m=l, x=below))

    @pl.when(sends_up)
    def _():
        for l in range(levels):
            pair = (n_send.at[0], n_recv.at[0])
            row = mem - ring
            send(msg.at[l, edge_part], q.at[row], pair, at(m=l, x=above))

    for p in peers:
        pair = (q_sem.at[0], q_sem.at[1])
        send(msg.at[p, edge_part], q.at[REACH + edge_row], pair, at(m=p))
    for v in range(3):
        q[REACH + edge_row, v] = msg[mem, v]

    pl.when(~late)(spread_on)

    settle(rbuf.at[pl.ds(1, nmem - 1), pl.ds(10, 6)], p1_sem.at[3], True)
    cells_of_row(1, 3)
    inner_row = REACH + mem
    for p in peers:
        pair = (q_sem.at[0], q_sem.at[1])
        send(msg.at[p, inner_part], q.at[REACH + inner_row, pl.ds(0, 2)], pair, at(m=p))
    for v in range(2):
        q[REACH + inner_row, v] = msg[mem, 3 + v]

    settle(means.at[pl.ds(0, nmem - 1)], m_sem.at[1], True)
    for d in range(nmem):
        means_ref[d] = means[d]
    settle(msg.at[pl.ds(0, nmem - 1)], q_sem.at[1], True)
    pl.when(sx > 0)(lambda: settle(q.at[pl.ds(0, REACH)], n_recv.at[0], True))
    pl.when(sx < nsx - 1)(lambda: settle(q.at[pl.ds(REACH + rows, REACH)], n_recv.at[1], True))

    table = gaspari_table(REACH)
    for d in range(nmem):
        row = d if d < ring else d + rows - nmem
        odd[d] = pltpu.roll(q[REACH + row, 2], LANES // 2, 1)

    def cells(row):
        inner = row - 2 * REACH
        side = odd[inner] if 0 <= inner < nmem else q[row, 2]
        return jnp.concatenate([q[row, 0], q[row, 1], side], axis=1)

    for i in range(rows):
        center = i + REACH
        lines = [cells(center)]
        for e in range(1, REACH + 1):
            lines.append(cells(center - e) + cells(center + e))
        out = None
        for f in range(REACH + 1):
            line = None
            for e in range(REACH + 1):
                weight = float(table[REACH + e, REACH + f])
                if weight != 0.0:
                    term = weight * lines[e]
                    line = term if line is None else line + term
            if f == 0:
                out = line
            else:
                out = out + pltpu.roll(line, f, 1) + pltpu.roll(line, width - f, 1)
        for c in range(2):
            z_ref[c, pl.ds(i, levels, stride=rows), :] = out[:, c * LANES : (c + 1) * LANES]

    settle(s2.at[pl.ds(1, len(others))], s2_sem.at[1], True)
    all_ref[...] = jnp.sum(s2[...], axis=0)

    settle(rbuf.at[pl.ds(1, nmem - 1)], p1_sem.at[0], False)
    pl.when(sy < nsy - 1)(lambda: settle(pack, e_send.at[0], False))
    pl.when(sy > 0)(lambda: settle(pack, e_send.at[1], False))
    settle(hsend.at[pl.ds(0, nmem - 1)], h_sem.at[0], False)
    settle(s1.at[pl.ds(1, ring - 1)], s1_sem.at[0], False)
    settle(mmsg.at[pl.ds(0, nmem - 1)], m_sem.at[0], False)
    settle(msg.at[pl.ds(0, nmem - 1)], q_sem.at[0], False)
    pl.when(sends_down | sends_up)(lambda: settle(q.at[pl.ds(0, levels)], n_send.at[0], False))
    settle(s2.at[pl.ds(1, len(others))], s2_sem.at[0], False)


def scale(count, z_ref, all_ref, means_ref, mean_ref, cov_ref):
    levels, rows, cols = cov_ref.shape
    spread = jnp.sum(all_ref[...], keepdims=True) * (1.0 / count)
    inverse = 1.0 / (spread + 1e-6)
    for k in range(levels):
        for c in range(cols // LANES):
            block = z_ref[c, pl.ds(k * rows, rows), :]
            cov_ref[k, :, pl.ds(c * LANES, LANES)] = block * inverse
    for i in range(rows):
        inner = 1 if REACH <= i < rows - REACH else 0
        source = i - REACH if inner else i % (rows - 2 * REACH)
        for c in range(cols // LANES):
            row = means_ref[source, pl.ds(2 * inner + c, 1), :]
            mean_ref[0, pl.ds(i, 1), pl.ds(c * LANES, LANES)] = row


def solution(mesh):
    nmem, nsx, nsy = (mesh.shape[name] for name in ("mem", "sx", "sy"))

    def local(child):
        members, levels, child_rows, child_cols = child.shape
        rows, cols = child_rows // 3, child_cols // 3
        f32 = jnp.float32
        dma = pltpu.SemaphoreType.DMA
        vmem = pl.BlockSpec(memory_space=pltpu.VMEM)
        vector = (SUB, LANES)
        z, total, means = pl.pallas_call(
            functools.partial(gather, nmem, nsx, nsy),
            out_shape=(
                jax.ShapeDtypeStruct((2, levels * rows, LANES), f32),
                jax.ShapeDtypeStruct((1, LANES), f32),
                jax.ShapeDtypeStruct((nmem, *vector), f32),
            ),
            in_specs=[pl.BlockSpec(memory_space=pltpu.MemorySpace.HBM)],
            out_specs=(vmem, vmem, vmem),
            scratch_shapes=[
                pltpu.VMEM((2, members, levels, child_rows // 2, child_cols), child.dtype),
                pltpu.VMEM((3 * LANES, LANES), child.dtype),
                pltpu.VMEM((2, members * levels * child_rows // 2, LANES), f32),
                pltpu.VMEM((2, nmem // 2, 16, *vector), f32),
                pltpu.VMEM((nmem, 16, *vector), f32),
                pltpu.VMEM((nmem, *vector), f32),
                pltpu.VMEM((nmem, *vector), f32),
                pltpu.VMEM((nmem, *vector), f32),
                pltpu.VMEM((nmem, *vector), f32),
                pltpu.VMEM((nmem, *vector), f32),
                pltpu.VMEM((4, nmem, *vector), f32),
                pltpu.VMEM((nmem * members, *vector), f32),
                pltpu.VMEM((4, *vector), f32),
                pltpu.VMEM((levels, *vector), f32),
                pltpu.VMEM((nmem, *vector), f32),
                pltpu.VMEM((levels, 5, *vector), f32),
                pltpu.VMEM((rows + 2 * REACH, 3, *vector), f32),
                pltpu.VMEM((nmem, *vector), f32),
                pltpu.VMEM((nmem // 2, 1, LANES), f32),
                pltpu.VMEM((2 * nsx * nsy, 1, LANES), f32),
                dma((2,)),
                dma((4,)),
                dma((2,)),
                dma((2,)),
                dma((2,)),
                dma((2,)),
                dma((2,)),
                dma((2,)),
                dma((1,)),
                dma((2,)),
                dma((2,)),
                pltpu.SemaphoreType.REGULAR((2,)),
            ],
            compiler_params=pltpu.CompilerParams(collective_id=0, has_side_effects=True, vmem_limit_bytes=VMEM_GRANT),
            name="gather",
        )(child)
        count = 4.0 * 81.0 * (members * nmem - 1) * levels * rows * nsx * cols * nsy
        return pl.pallas_call(
            functools.partial(scale, count),
            out_shape=(
                jax.ShapeDtypeStruct((levels // nmem, rows, cols), f32),
                jax.ShapeDtypeStruct((levels, rows, cols), f32),
            ),
            in_specs=[vmem, vmem, vmem],
            out_specs=(vmem, vmem),
            compiler_params=pltpu.CompilerParams(vmem_limit_bytes=8 << 20),
            name="scale",
        )(z, total, means)

    return jax.shard_map(
        local,
        mesh=mesh,
        in_specs=(P("mem", None, "sx", "sy"),),
        out_specs=(P("mem", "sx", "sy"), P("mem", "sx", "sy")),
        check_vma=False,
    )
```

```python
import functools

import jax
import jax.numpy as jnp
import numpy as np
from jax import lax
from jax.experimental import pallas as pl
from jax.experimental.pallas import tpu as pltpu
from jax.sharding import PartitionSpec as P

MESH = pl.DeviceIdType.MESH
REACH = 4
LANES = 128
SUB = 8
VMEM_GRANT = 55_500_000


def gaspari_table(reach):
    offsets = np.arange(-reach, reach + 1) * 1.0
    dist = np.sqrt(offsets[:, None] ** 2 + offsets[None, :] ** 2) / 2.5
    near = -0.25 * dist**5 + 0.5 * dist**4 + 0.625 * dist**3 - 5.0 / 3.0 * dist**2 + 1.0
    safe = np.maximum(dist, 0.001)
    far = (
        dist**5 / 12.0
        - 0.5 * dist**4
        + 0.625 * dist**3
        + 5.0 / 3.0 * dist**2
        - 5.0 * dist
        + 4.0
        - 2.0 / (3.0 * safe)
    )
    table = np.where(dist <= 1.0, near, np.where(dist < 2.0, far, 0.0))
    return table / table.sum()


def gather(
    nmem,
    nsx,
    nsy,
    child_ref,
    z_ref,
    all_ref,
    means_ref,
    xbuf,
    pick,
    ybuf,
    psend,
    rbuf,
    pack,
    from_left,
    from_right,
    hsend,
    hbuf,
    abuf,
    sbuf,
    mbuf,
    mmsg,
    means,
    msg,
    q,
    odd,
    s1,
    s2,
    ld_sem,
    p1_sem,
    e_send,
    e_recv,
    h_sem,
    s1_sem,
    m_sem,
    q_sem,
    n_send,
    n_recv,
    s2_sem,
    known,
):
    members, levels, child_rows, child_cols = child_ref.shape
    rows = child_rows // 3
    half_rows = child_rows // 2
    mem = lax.axis_index("mem")
    sx = lax.axis_index("sx")
    sy = lax.axis_index("sy")
    total_members = members * nmem
    ring = nmem // 2
    z, y = mem // ring, lax.rem(mem, ring)

    def at(m=None, x=None, y=None):
        return {
            "mem": mem if m is None else m,
            "sx": sx if x is None else x,
            "sy": sy if y is None else y,
        }

    loads = []
    for half, owner_z in enumerate((1 - z, z)):
        first = pl.multiple_of(owner_z * half_rows, SUB)
        copy = pltpu.make_async_copy(
            child_ref.at[:, :, pl.ds(first, half_rows), :], xbuf.at[half], ld_sem.at[half]
        )
        copy.start()
        loads.append(copy)

    steps = [(1, 0), (1, 1), (1, 3), (1, 2), (0, 2), (0, 1), (0, 3)]
    spots = [lax.rem(y + b, ring) for _, b in steps]
    peers = [lax.rem(z + a, 2) * ring + spot for (a, _), spot in zip(steps, spots)]
    plane = [(a, b) for a in range(nsx) for b in range(nsy) if (a, b) != (0, 0)]
    plane_peers = [(lax.rem(sx + a, nsx), lax.rem(sy + b, nsy)) for a, b in plane]
    above, below = lax.rem(sx + 1, nsx), lax.rem(sx + nsx - 1, nsx)

    def send(src, dst, pair, device):
        copy = pltpu.make_async_remote_copy(
            src_ref=src,
            dst_ref=dst,
            send_sem=pair[0],
            recv_sem=pair[1],
            device_id=device,
            device_id_type=MESH,
        )
        copy.start()

    def settle(ref, sem, received):
        copy = pltpu.make_async_remote_copy(
            src_ref=ref,
            dst_ref=ref,
            send_sem=sem,
            recv_sem=sem,
            device_id=at(m=peers[0]),
            device_id_type=MESH,
        )
        if received:
            copy.wait_recv()
        else:
            copy.wait_send()

    def greet(sem, friend):
        pl.semaphore_signal(sem, inc=1, device_id=friend, device_id_type=MESH)

    fellows = (mem, peers[0])

    def greet_around(sem, whom):
        for a in (-1, 0, 1):
            for b in (-1, 0, 1):
                if (a, b) != (0, 0):
                    inside = (sx + a >= 0) & (sx + a < nsx) & (sy + b >= 0) & (sy + b < nsy)
                    x, y2 = lax.rem(sx + a + nsx, nsx), lax.rem(sy + b + nsy, nsy)

                    @pl.when(inside)
                    def _():
                        for m in whom:
                            greet(sem, at(m=m, x=x, y=y2))

    tiles_x = 3 - jnp.where(sx == 0, 1, 0) - jnp.where(sx == nsx - 1, 1, 0)
    tiles_y = 3 - jnp.where(sy == 0, 1, 0) - jnp.where(sy == nsy - 1, 1, 0)
    around = tiles_x * tiles_y - 1
    barrier = pltpu.get_barrier_semaphore()
    for p in peers:
        greet(barrier, at(m=p))
    greet_around(barrier, fellows)

    zero = jnp.zeros((SUB, LANES), jnp.float32)

    width = 3 * LANES
    r_ids = lax.broadcasted_iota(jnp.int32, (width, LANES), 0)
    c_ids = lax.broadcasted_iota(jnp.int32, (width, LANES), 1)
    off = r_ids - 3 * c_ids
    pick[...] = jnp.where((off >= 0) & (off <= 2), 1.0, 0.0).astype(jnp.bfloat16)

    def post(first, count, n, sem):
        part = pl.ds(first, count)
        send(
            psend.at[1 - steps[n][0], spots[n], part],
            rbuf.at[n + 1, part],
            (p1_sem.at[0], p1_sem.at[sem]),
            at(m=peers[n]),
        )

    within = zero
    for half, owner_z in enumerate((1 - z, z)):
        loads[half].wait()
        for c in range(2):
            ybuf[c] = jnp.dot(
                xbuf[half, :, :, :, pl.ds(c * width, width)].reshape(-1, width),
                pick[...],
                preferred_element_type=jnp.float32,
            )
        for i in range(rows // 2):
            for c in range(2):
                p = []
                for m in range(members):
                    total = None
                    for a in range(3):
                        start = m * levels * half_rows + 3 * i + a
                        line = ybuf[c, pl.ds(start, levels, stride=half_rows), :]
                        total = line if total is None else total + line
                    p.append(total)
                up, down = p[0] + p[1], p[2] + p[3]
                left, right = p[0] - p[1], p[2] - p[3]
                owner, inside = i % ring, i // ring
                i2 = inside + owner_z - 2 * inside * owner_z
                psend[half, owner, 2 * i2 + c] = up + down
                for j, value in enumerate((up - down, left + right, left - right)):
                    psend[half, owner, 4 + 6 * i2 + 2 * j + c] = value
                    within += value * value
    pl.semaphore_wait(barrier, len(peers) + 2 * around)
    greet_around(known.at[0], (mem,))
    for n in (3, 1, 2, 4, 0, 5, 6):
        post(0, 4, n, 1)

    def clear_rows(first):
        for row in range(first, first + REACH):
            for v in range(3):
                q[row, v] = zero

    def clear_side(ref):
        for d in range(nmem):
            ref[d] = zero

    pl.when(sx == 0)(lambda: clear_rows(0))
    pl.when(sx == nsx - 1)(lambda: clear_rows(REACH + rows))
    pl.when(sy == 0)(lambda: clear_side(from_left))
    pl.when(sy == nsy - 1)(lambda: clear_side(from_right))

    lane = lax.broadcasted_iota(jnp.int32, (SUB, LANES), 1)
    for d in range(nmem):
        half, owner = d // ring, d % ring
        packed = zero
        for j in range(members):
            for i2 in range(2):
                shift = 8 * j + 64 * i2
                k = 2 * i2 if j == 0 else 2 + 6 * i2 + 2 * j
                both = jnp.where(
                    lane < LANES // 2, psend[half, owner, k], psend[half, owner, k + 1]
                )
                if shift:
                    both = pltpu.roll(both, shift, 1)
                mine = ((lane - shift + 4 + LANES) & (LANES - 1)) < 8
                packed = jnp.where(mine, both, packed)
        pack[d] = packed

    @pl.when(sy < nsy - 1)
    def _():
        send(pack, from_left, (e_send.at[0], e_recv.at[0]), at(y=lax.rem(sy + 1, nsy)))

    @pl.when(sy > 0)
    def _():
        send(pack, from_right, (e_send.at[1], e_recv.at[1]), at(y=lax.rem(sy + nsy - 1, nsy)))

    late = sy + 2 * (sx // 2) >= 4

    def post_edge_rows(some):
        for n in some:
            post(4, 6, n, 2)

    pl.when(~late)(lambda: post_edge_rows(range(nmem - 1)))
    for k in range(16):
        rbuf[0, k] = psend[1, y, k]

    pl.semaphore_wait(known.at[0], around)
    greet_around(known.at[1], (mem,))
    pl.when(late)(lambda: post_edge_rows(range(7)))

    pl.when(sy > 0)(lambda: settle(from_left, e_recv.at[0], True))
    pl.when(sy < nsy - 1)(lambda: settle(from_right, e_recv.at[1], True))
    for d in range(nmem):
        hsend[d] = jnp.where((lane & 4) == 0, from_right[d], from_left[d])

    def pass_edges():
        for n, (p, spot) in enumerate(zip(peers, spots)):
            owner = (1 - steps[n][0]) * ring + spot
            send(hsend.at[owner], hbuf.at[n + 1], (h_sem.at[0], h_sem.at[1]), at(m=p))

    pl.when(~late)(pass_edges)
    hbuf[0] = hsend[ring + y]

    settle(rbuf.at[pl.ds(1, nmem - 1), pl.ds(0, 4)], p1_sem.at[1], True)
    var = within
    for v in range(4):
        total = rbuf[0, v]
        for o in range(1, nmem):
            total += rbuf[o, v]
        mbuf[v] = total * (1.0 / (9.0 * total_members))
        middle = total * (1.0 / nmem)
        for o in range(nmem):
            anom = rbuf[o, v] - middle
            abuf[v, o] = anom
            var += anom * anom
    s1[0] = jnp.sum(var, axis=0, keepdims=True)
    for n, p in enumerate(peers[ring:]):
        send(s1.at[0], s1.at[n + 1], (s1_sem.at[0], s1_sem.at[1]), at(m=p))
    pl.when(late)(pass_edges)
    def post_inner_rows():
        for n in range(nmem - 1):
            post(10, 6, n, 3)

    pl.when(~late)(post_inner_rows)
    for l in range(levels):
        mmsg[l] = zero
        for v in range(4):
            mmsg[l, pl.ds(v, 1), :] = mbuf[v, pl.ds(l, 1), :]
    for p in peers:
        send(mmsg.at[p], means.at[mem], (m_sem.at[0], m_sem.at[1]), at(m=p))
    means[mem] = mmsg[mem]

    factor = 1.0 / (4.0 * 81.0 * (total_members - 1))

    def covariances(v, vectors):
        acc = [zero] * levels
        for ref, index in vectors:
            anom = ref[index]
            for l in range(levels):
                acc[l] += anom * ref[(*index, pl.ds(l, 1), slice(None))]
        for l in range(levels):
            msg[l, v] = acc[l] * factor

    def cells_of_row(i2, first):
        def column(c, carry):
            vectors = []
            for o in range(nmem):
                vectors.append((abuf, (2 * i2 + c, o)))
                vectors += [(rbuf, (o, 4 + 6 * i2 + 2 * j + c)) for j in range(members - 1)]
            covariances(first + c, vectors)
            return carry

        lax.fori_loop(0, 2, column, 0)

    others = [(m, a, b) for a, b in plane_peers for m in fellows] + [(peers[0], sx, sy)]

    def spread_on():
        settle(s1.at[pl.ds(1, ring - 1)], s1_sem.at[1], True)
        pl.semaphore_wait(known.at[1], around)
        s2[0] = jnp.sum(s1[...], axis=0)
        for n, (m, a, b) in enumerate(others):
            send(s2.at[0], s2.at[n + 1], (s2_sem.at[0], s2_sem.at[1]), at(m, a, b))

    def edge_rows_arrived():
        settle(rbuf.at[pl.ds(1, nmem - 1), pl.ds(4, 6)], p1_sem.at[2], True)

    @pl.when(late)
    def _():
        edge_rows_arrived()
        post_inner_rows()
        spread_on()

    pl.when(~late)(edge_rows_arrived)
    cells_of_row(0, 0)
    settle(hbuf.at[pl.ds(1, nmem - 1)], h_sem.at[1], True)
    total = hbuf[0]
    for o in range(1, nmem):
        total += hbuf[o]
    middle = total * (1.0 / nmem)
    for o in range(nmem):
        sbuf[members * o] = hbuf[o] - middle
        for j in range(1, members):
            sbuf[members * o + j] = pltpu.roll(hbuf[o], LANES - 8 * j, 1)
    covariances(2, [(sbuf, (t,)) for t in range(total_members)])

    edge_row = mem + z * (rows - nmem)
    sends_down = (z == 0) & (sx > 0)
    sends_up = (z == 1) & (sx < nsx - 1)
    edge_part, inner_part = pl.ds(0, 3), pl.ds(3, 2)

    @pl.when(sends_down)
    def _():
        for l in range(levels):
            pair = (n_send.at[0], n_recv.at[1])
            row = REACH + rows + mem
            send(msg.at[l, edge_part], q.at[row], pair, at(m=l, x=below))

    @pl.when(sends_up)
    def _():
        for l in range(levels):
            pair = (n_send.at[0], n_recv.at[0])
            row = mem - ring
            send(msg.at[l, edge_part], q.at[row], pair, at(m=l, x=above))

    for p in peers:
        pair = (q_sem.at[0], q_sem.at[1])
        send(msg.at[p, edge_part], q.at[REACH + edge_row], pair, at(m=p))
    for v in range(3):
        q[REACH + edge_row, v] = msg[mem, v]

    pl.when(~late)(spread_on)

    settle(rbuf.at[pl.ds(1, nmem - 1), pl.ds(10, 6)], p1_sem.at[3], True)
    cells_of_row(1, 3)
    inner_row = REACH + mem
    for p in peers:
        pair = (q_sem.at[0], q_sem.at[1])
        send(msg.at[p, inner_part], q.at[REACH + inner_row, pl.ds(0, 2)], pair, at(m=p))
    for v in range(2):
        q[REACH + inner_row, v] = msg[mem, 3 + v]

    settle(means.at[pl.ds(0, nmem - 1)], m_sem.at[1], True)
    for d in range(nmem):
        means_ref[d] = means[d]
    settle(msg.at[pl.ds(0, nmem - 1)], q_sem.at[1], True)
    pl.when(sx > 0)(lambda: settle(q.at[pl.ds(0, REACH)], n_recv.at[0], True))
    pl.when(sx < nsx - 1)(lambda: settle(q.at[pl.ds(REACH + rows, REACH)], n_recv.at[1], True))

    table = gaspari_table(REACH)
    for d in range(nmem):
        row = d if d < ring else d + rows - nmem
        odd[d] = pltpu.roll(q[REACH + row, 2], LANES // 2, 1)

    def cells(row):
        inner = row - 2 * REACH
        side = odd[inner] if 0 <= inner < nmem else q[row, 2]
        return jnp.concatenate([q[row, 0], q[row, 1], side], axis=1)

    for i in range(rows):
        center = i + REACH
        lines = [cells(center)]
        for e in range(1, REACH + 1):
            lines.append(cells(center - e) + cells(center + e))
        out = None
        for f in range(REACH + 1):
            line = None
            for e in range(REACH + 1):
                weight = float(table[REACH + e, REACH + f])
                if weight != 0.0:
                    term = weight * lines[e]
                    line = term if line is None else line + term
            if f == 0:
                out = line
            else:
                out = out + pltpu.roll(line, f, 1) + pltpu.roll(line, width - f, 1)
        for c in range(2):
            z_ref[c, pl.ds(i, levels, stride=rows), :] = out[:, c * LANES : (c + 1) * LANES]

    settle(s2.at[pl.ds(1, len(others))], s2_sem.at[1], True)
    all_ref[...] = jnp.sum(s2[...], axis=0)

    settle(rbuf.at[pl.ds(1, nmem - 1)], p1_sem.at[0], False)
    pl.when(sy < nsy - 1)(lambda: settle(pack, e_send.at[0], False))
    pl.when(sy > 0)(lambda: settle(pack, e_send.at[1], False))
    settle(hsend.at[pl.ds(0, nmem - 1)], h_sem.at[0], False)
    settle(s1.at[pl.ds(1, ring - 1)], s1_sem.at[0], False)
    settle(mmsg.at[pl.ds(0, nmem - 1)], m_sem.at[0], False)
    settle(msg.at[pl.ds(0, nmem - 1)], q_sem.at[0], False)
    pl.when(sends_down | sends_up)(lambda: settle(q.at[pl.ds(0, levels)], n_send.at[0], False))
    settle(s2.at[pl.ds(1, len(others))], s2_sem.at[0], False)


def scale(count, z_ref, all_ref, means_ref, mean_ref, cov_ref):
    levels, rows, cols = cov_ref.shape
    spread = jnp.sum(all_ref[...], keepdims=True) * (1.0 / count)
    inverse = 1.0 / (spread + 1e-6)
    for k in range(levels):
        for c in range(cols // LANES):
            block = z_ref[c, pl.ds(k * rows, rows), :]
            cov_ref[k, :, pl.ds(c * LANES, LANES)] = block * inverse
    for i in range(rows):
        inner = 1 if REACH <= i < rows - REACH else 0
        source = i - REACH if inner else i % (rows - 2 * REACH)
        for c in range(cols // LANES):
            row = means_ref[source, pl.ds(2 * inner + c, 1), :]
            mean_ref[0, pl.ds(i, 1), pl.ds(c * LANES, LANES)] = row


def solution(mesh):
    nmem, nsx, nsy = (mesh.shape[name] for name in ("mem", "sx", "sy"))

    def local(child):
        members, levels, child_rows, child_cols = child.shape
        rows, cols = child_rows // 3, child_cols // 3
        f32 = jnp.float32
        dma = pltpu.SemaphoreType.DMA
        vmem = pl.BlockSpec(memory_space=pltpu.VMEM)
        vector = (SUB, LANES)
        z, total, means = pl.pallas_call(
            functools.partial(gather, nmem, nsx, nsy),
            out_shape=(
                jax.ShapeDtypeStruct((2, levels * rows, LANES), f32),
                jax.ShapeDtypeStruct((1, LANES), f32),
                jax.ShapeDtypeStruct((nmem, *vector), f32),
            ),
            in_specs=[pl.BlockSpec(memory_space=pltpu.MemorySpace.HBM)],
            out_specs=(vmem, vmem, vmem),
            scratch_shapes=[
                pltpu.VMEM((2, members, levels, child_rows // 2, child_cols), child.dtype),
                pltpu.VMEM((3 * LANES, LANES), child.dtype),
                pltpu.VMEM((2, members * levels * child_rows // 2, LANES), f32),
                pltpu.VMEM((2, nmem // 2, 16, *vector), f32),
                pltpu.VMEM((nmem, 16, *vector), f32),
                pltpu.VMEM((nmem, *vector), f32),
                pltpu.VMEM((nmem, *vector), f32),
                pltpu.VMEM((nmem, *vector), f32),
                pltpu.VMEM((nmem, *vector), f32),
                pltpu.VMEM((nmem, *vector), f32),
                pltpu.VMEM((4, nmem, *vector), f32),
                pltpu.VMEM((nmem * members, *vector), f32),
                pltpu.VMEM((4, *vector), f32),
                pltpu.VMEM((levels, *vector), f32),
                pltpu.VMEM((nmem, *vector), f32),
                pltpu.VMEM((levels, 5, *vector), f32),
                pltpu.VMEM((rows + 2 * REACH, 3, *vector), f32),
                pltpu.VMEM((nmem, *vector), f32),
                pltpu.VMEM((nmem // 2, 1, LANES), f32),
                pltpu.VMEM((2 * nsx * nsy, 1, LANES), f32),
                dma((2,)),
                dma((4,)),
                dma((2,)),
                dma((2,)),
                dma((2,)),
                dma((2,)),
                dma((2,)),
                dma((2,)),
                dma((1,)),
                dma((2,)),
                dma((2,)),
                pltpu.SemaphoreType.REGULAR((2,)),
            ],
            compiler_params=pltpu.CompilerParams(collective_id=0, has_side_effects=True, vmem_limit_bytes=VMEM_GRANT),
            name="gather",
        )(child)
        count = 4.0 * 81.0 * (members * nmem - 1) * levels * rows * nsx * cols * nsy
        return pl.pallas_call(
            functools.partial(scale, count),
            out_shape=(
                jax.ShapeDtypeStruct((levels // nmem, rows, cols), f32),
                jax.ShapeDtypeStruct((levels, rows, cols), f32),
            ),
            in_specs=[vmem, vmem, vmem],
            out_specs=(vmem, vmem),
            compiler_params=pltpu.CompilerParams(vmem_limit_bytes=8 << 20),
            name="scale",
        )(z, total, means)

    return jax.shard_map(
        local,
        mesh=mesh,
        in_specs=(P("mem", None, "sx", "sy"),),
        out_specs=(P("mem", "sx", "sy"), P("mem", "sx", "sy")),
        check_vma=False,
    )
```

```python
import functools

import jax
import jax.numpy as jnp
import numpy as np
from jax import lax
from jax.experimental import pallas as pl
from jax.experimental.pallas import tpu as pltpu
from jax.sharding import PartitionSpec as P

MESH = pl.DeviceIdType.MESH
REACH = 4
LANES = 128
SUB = 8
VMEM_GRANT = 55_500_000


def gaspari_table(reach):
    offsets = np.arange(-reach, reach + 1) * 1.0
    dist = np.sqrt(offsets[:, None] ** 2 + offsets[None, :] ** 2) / 2.5
    near = -0.25 * dist**5 + 0.5 * dist**4 + 0.625 * dist**3 - 5.0 / 3.0 * dist**2 + 1.0
    safe = np.maximum(dist, 0.001)
    far = (
        dist**5 / 12.0
        - 0.5 * dist**4
        + 0.625 * dist**3
        + 5.0 / 3.0 * dist**2
        - 5.0 * dist
        + 4.0
        - 2.0 / (3.0 * safe)
    )
    table = np.where(dist <= 1.0, near, np.where(dist < 2.0, far, 0.0))
    return table / table.sum()


def gather(
    nmem,
    nsx,
    nsy,
    child_ref,
    z_ref,
    all_ref,
    means_ref,
    xbuf,
    pick,
    ybuf,
    psend,
    rbuf,
    pack,
    from_left,
    from_right,
    hsend,
    hbuf,
    abuf,
    sbuf,
    mbuf,
    mmsg,
    means,
    msg,
    q,
    odd,
    s1,
    s2,
    ld_sem,
    p1_sem,
    e_send,
    e_recv,
    h_sem,
    s1_sem,
    m_sem,
    q_sem,
    n_send,
    n_recv,
    s2_sem,
    known,
):
    members, levels, child_rows, child_cols = child_ref.shape
    rows = child_rows // 3
    half_rows = child_rows // 2
    mem = lax.axis_index("mem")
    sx = lax.axis_index("sx")
    sy = lax.axis_index("sy")
    total_members = members * nmem
    ring = nmem // 2
    z, y = mem // ring, lax.rem(mem, ring)

    def at(m=None, x=None, y=None):
        return {
            "mem": mem if m is None else m,
            "sx": sx if x is None else x,
            "sy": sy if y is None else y,
        }

    steps = [(1, 0), (1, 1), (1, 3), (1, 2), (0, 2), (0, 1), (0, 3)]
    spots = [lax.rem(y + b, ring) for _, b in steps]
    peers = [lax.rem(z + a, 2) * ring + spot for (a, _), spot in zip(steps, spots)]
    plane = [(a, b) for a in range(nsx) for b in range(nsy) if (a, b) != (0, 0)]
    plane_peers = [(lax.rem(sx + a, nsx), lax.rem(sy + b, nsy)) for a, b in plane]
    above, below = lax.rem(sx + 1, nsx), lax.rem(sx + nsx - 1, nsx)

    def send(src, dst, pair, device):
        copy = pltpu.make_async_remote_copy(
            src_ref=src,
            dst_ref=dst,
            send_sem=pair[0],
            recv_sem=pair[1],
            device_id=device,
            device_id_type=MESH,
        )
        copy.start()

    def settle(ref, sem, received):
        copy = pltpu.make_async_remote_copy(
            src_ref=ref,
            dst_ref=ref,
            send_sem=sem,
            recv_sem=sem,
            device_id=at(m=peers[0]),
            device_id_type=MESH,
        )
        if received:
            copy.wait_recv()
        else:
            copy.wait_send()

    def greet(sem, friend):
        pl.semaphore_signal(sem, inc=1, device_id=friend, device_id_type=MESH)

    fellows = (mem, peers[0])

    def greet_around(sem, whom):
        for a in (-1, 0, 1):
            for b in (-1, 0, 1):
                if (a, b) != (0, 0):
                    inside = (sx + a >= 0) & (sx + a < nsx) & (sy + b >= 0) & (sy + b < nsy)
                    x, y2 = lax.rem(sx + a + nsx, nsx), lax.rem(sy + b + nsy, nsy)

                    @pl.when(inside)
                    def _():
                        for m in whom:
                            greet(sem, at(m=m, x=x, y=y2))

    tiles_x = 3 - jnp.where(sx == 0, 1, 0) - jnp.where(sx == nsx - 1, 1, 0)
    tiles_y = 3 - jnp.where(sy == 0, 1, 0) - jnp.where(sy == nsy - 1, 1, 0)
    around = tiles_x * tiles_y - 1
    barrier = pltpu.get_barrier_semaphore()
    for p in peers:
        greet(barrier, at(m=p))

    loads = []
    for half, owner_z in enumerate((1 - z, z)):
        first = pl.multiple_of(owner_z * half_rows, SUB)
        copy = pltpu.make_async_copy(
            child_ref.at[:, :, pl.ds(first, half_rows), :], xbuf.at[half], ld_sem.at[half]
        )
        copy.start()
        loads.append(copy)

    greet_around(barrier, fellows)

    zero = jnp.zeros((SUB, LANES), jnp.float32)

    width = 3 * LANES
    r_ids = lax.broadcasted_iota(jnp.int32, (width, LANES), 0)
    c_ids = lax.broadcasted_iota(jnp.int32, (width, LANES), 1)
    off = r_ids - 3 * c_ids
    pick[...] = jnp.where((off >= 0) & (off <= 2), 1.0, 0.0).astype(jnp.bfloat16)

    def post(first, count, n, sem):
        part = pl.ds(first, count)
        send(
            psend.at[1 - steps[n][0], spots[n], part],
            rbuf.at[n + 1, part],
            (p1_sem.at[0], p1_sem.at[sem]),
            at(m=peers[n]),
        )

    within = zero
    for half, owner_z in enumerate((1 - z, z)):
        loads[half].wait()
        for c in range(2):
            ybuf[c] = jnp.dot(
                xbuf[half, :, :, :, pl.ds(c * width, width)].reshape(-1, width),
                pick[...],
                preferred_element_type=jnp.float32,
            )
        for i in range(rows // 2):
            for c in range(2):
                p = []
                for m in range(members):
                    total = None
                    for a in range(3):
                        start = m * levels * half_rows + 3 * i + a
                        line = ybuf[c, pl.ds(start, levels, stride=half_rows), :]
                        total = line if total is None else total + line
                    p.append(total)
                up, down = p[0] + p[1], p[2] + p[3]
                left, right = p[0] - p[1], p[2] - p[3]
                owner, inside = i % ring, i // ring
                i2 = inside + owner_z - 2 * inside * owner_z
                psend[half, owner, 2 * i2 + c] = up + down
                for j, value in enumerate((up - down, left + right, left - right)):
                    psend[half, owner, 4 + 6 * i2 + 2 * j + c] = value
                    within += value * value
    pl.semaphore_wait(barrier, len(peers) + 2 * around)
    greet_around(known.at[0], (mem,))
    for n in (3, 1, 2, 4, 0, 5, 6):
        post(0, 4, n, 1)

    def clear_rows(first):
        for row in range(first, first + REACH):
            for v in range(3):
                q[row, v] = zero

    def clear_side(ref):
        for d in range(nmem):
            ref[d] = zero

    pl.when(sx == 0)(lambda: clear_rows(0))
    pl.when(sx == nsx - 1)(lambda: clear_rows(REACH + rows))
    pl.when(sy == 0)(lambda: clear_side(from_left))
    pl.when(sy == nsy - 1)(lambda: clear_side(from_right))

    lane = lax.broadcasted_iota(jnp.int32, (SUB, LANES), 1)
    for d in range(nmem):
        half, owner = d // ring, d % ring
        packed = zero
        for j in range(members):
            for i2 in range(2):
                shift = 8 * j + 64 * i2
                k = 2 * i2 if j == 0 else 2 + 6 * i2 + 2 * j
                both = jnp.where(
                    lane < LANES // 2, psend[half, owner, k], psend[half, owner, k + 1]
                )
                if shift:
                    both = pltpu.roll(both, shift, 1)
                mine = ((lane - shift + 4 + LANES) & (LANES - 1)) < 8
                packed = jnp.where(mine, both, packed)
        pack[d] = packed

    @pl.when(sy < nsy - 1)
    def _():
        send(pack, from_left, (e_send.at[0], e_recv.at[0]), at(y=lax.rem(sy + 1, nsy)))

    @pl.when(sy > 0)
    def _():
        send(pack, from_right, (e_send.at[1], e_recv.at[1]), at(y=lax.rem(sy + nsy - 1, nsy)))

    late = sy + 2 * (sx // 2) >= 4

    def post_edge_rows(some):
        for n in some:
            post(4, 6, n, 2)

    pl.when(~late)(lambda: post_edge_rows(range(nmem - 1)))
    for k in range(16):
        rbuf[0, k] = psend[1, y, k]

    pl.semaphore_wait(known.at[0], around)
    greet_around(known.at[1], (mem,))
    pl.when(late)(lambda: post_edge_rows(range(7)))

    pl.when(sy > 0)(lambda: settle(from_left, e_recv.at[0], True))
    pl.when(sy < nsy - 1)(lambda: settle(from_right, e_recv.at[1], True))
    for d in range(nmem):
        hsend[d] = jnp.where((lane & 4) == 0, from_right[d], from_left[d])

    def pass_edges():
        for n, (p, spot) in enumerate(zip(peers, spots)):
            owner = (1 - steps[n][0]) * ring + spot
            send(hsend.at[owner], hbuf.at[n + 1], (h_sem.at[0], h_sem.at[1]), at(m=p))

    pl.when(~late)(pass_edges)
    hbuf[0] = hsend[ring + y]

    settle(rbuf.at[pl.ds(1, nmem - 1), pl.ds(0, 4)], p1_sem.at[1], True)
    var = within
    for v in range(4):
        total = rbuf[0, v]
        for o in range(1, nmem):
            total += rbuf[o, v]
        mbuf[v] = total * (1.0 / (9.0 * total_members))
        middle = total * (1.0 / nmem)
        for o in range(nmem):
            anom = rbuf[o, v] - middle
            abuf[v, o] = anom
            var += anom * anom
    s1[0] = jnp.sum(var, axis=0, keepdims=True)
    for n, p in enumerate(peers[ring:]):
        send(s1.at[0], s1.at[n + 1], (s1_sem.at[0], s1_sem.at[1]), at(m=p))
    pl.when(late)(pass_edges)
    def post_inner_rows():
        for n in range(nmem - 1):
            post(10, 6, n, 3)

    pl.when(~late)(post_inner_rows)
    for l in range(levels):
        mmsg[l] = zero
        for v in range(4):
            mmsg[l, pl.ds(v, 1), :] = mbuf[v, pl.ds(l, 1), :]
    for p in peers:
        send(mmsg.at[p], means.at[mem], (m_sem.at[0], m_sem.at[1]), at(m=p))
    means[mem] = mmsg[mem]

    factor = 1.0 / (4.0 * 81.0 * (total_members - 1))

    def covariances(v, vectors):
        acc = [zero] * levels
        for ref, index in vectors:
            anom = ref[index]
            for l in range(levels):
                acc[l] += anom * ref[(*index, pl.ds(l, 1), slice(None))]
        for l in range(levels):
            msg[l, v] = acc[l] * factor

    def cells_of_row(i2, first):
        def column(c, carry):
            vectors = []
            for o in range(nmem):
                vectors.append((abuf, (2 * i2 + c, o)))
                vectors += [(rbuf, (o, 4 + 6 * i2 + 2 * j + c)) for j in range(members - 1)]
            covariances(first + c, vectors)
            return carry

        lax.fori_loop(0, 2, column, 0)

    others = [(m, a, b) for a, b in plane_peers for m in fellows] + [(peers[0], sx, sy)]

    def spread_on():
        settle(s1.at[pl.ds(1, ring - 1)], s1_sem.at[1], True)
        pl.semaphore_wait(known.at[1], around)
        s2[0] = jnp.sum(s1[...], axis=0)
        for n, (m, a, b) in enumerate(others):
            send(s2.at[0], s2.at[n + 1], (s2_sem.at[0], s2_sem.at[1]), at(m, a, b))

    def edge_rows_arrived():
        settle(rbuf.at[pl.ds(1, nmem - 1), pl.ds(4, 6)], p1_sem.at[2], True)

    @pl.when(late)
    def _():
        edge_rows_arrived()
        post_inner_rows()
        spread_on()

    pl.when(~late)(edge_rows_arrived)
    cells_of_row(0, 0)
    settle(hbuf.at[pl.ds(1, nmem - 1)], h_sem.at[1], True)
    total = hbuf[0]
    for o in range(1, nmem):
        total += hbuf[o]
    middle = total * (1.0 / nmem)
    for o in range(nmem):
        sbuf[members * o] = hbuf[o] - middle
        for j in range(1, members):
            sbuf[members * o + j] = pltpu.roll(hbuf[o], LANES - 8 * j, 1)
    covariances(2, [(sbuf, (t,)) for t in range(total_members)])

    edge_row = mem + z * (rows - nmem)
    sends_down = (z == 0) & (sx > 0)
    sends_up = (z == 1) & (sx < nsx - 1)
    edge_part, inner_part = pl.ds(0, 3), pl.ds(3, 2)

    @pl.when(sends_down)
    def _():
        for l in range(levels):
            pair = (n_send.at[0], n_recv.at[1])
            row = REACH + rows + mem
            send(msg.at[l, edge_part], q.at[row], pair, at(m=l, x=below))

    @pl.when(sends_up)
    def _():
        for l in range(levels):
            pair = (n_send.at[0], n_recv.at[0])
            row = mem - ring
            send(msg.at[l, edge_part], q.at[row], pair, at(m=l, x=above))

    for p in peers:
        pair = (q_sem.at[0], q_sem.at[1])
        send(msg.at[p, edge_part], q.at[REACH + edge_row], pair, at(m=p))
    for v in range(3):
        q[REACH + edge_row, v] = msg[mem, v]

    pl.when(~late)(spread_on)

    settle(rbuf.at[pl.ds(1, nmem - 1), pl.ds(10, 6)], p1_sem.at[3], True)
    cells_of_row(1, 3)
    inner_row = REACH + mem
    for p in peers:
        pair = (q_sem.at[0], q_sem.at[1])
        send(msg.at[p, inner_part], q.at[REACH + inner_row, pl.ds(0, 2)], pair, at(m=p))
    for v in range(2):
        q[REACH + inner_row, v] = msg[mem, 3 + v]

    settle(means.at[pl.ds(0, nmem - 1)], m_sem.at[1], True)
    for d in range(nmem):
        means_ref[d] = means[d]
    settle(msg.at[pl.ds(0, nmem - 1)], q_sem.at[1], True)
    pl.when(sx > 0)(lambda: settle(q.at[pl.ds(0, REACH)], n_recv.at[0], True))
    pl.when(sx < nsx - 1)(lambda: settle(q.at[pl.ds(REACH + rows, REACH)], n_recv.at[1], True))

    table = gaspari_table(REACH)
    for d in range(nmem):
        row = d if d < ring else d + rows - nmem
        odd[d] = pltpu.roll(q[REACH + row, 2], LANES // 2, 1)

    def cells(row):
        inner = row - 2 * REACH
        side = odd[inner] if 0 <= inner < nmem else q[row, 2]
        return jnp.concatenate([q[row, 0], q[row, 1], side], axis=1)

    for i in range(rows):
        center = i + REACH
        lines = [cells(center)]
        for e in range(1, REACH + 1):
            lines.append(cells(center - e) + cells(center + e))
        out = None
        for f in range(REACH + 1):
            line = None
            for e in range(REACH + 1):
                weight = float(table[REACH + e, REACH + f])
                if weight != 0.0:
                    term = weight * lines[e]
                    line = term if line is None else line + term
            if f == 0:
                out = line
            else:
                out = out + pltpu.roll(line, f, 1) + pltpu.roll(line, width - f, 1)
        for c in range(2):
            z_ref[c, pl.ds(i, levels, stride=rows), :] = out[:, c * LANES : (c + 1) * LANES]

    settle(s2.at[pl.ds(1, len(others))], s2_sem.at[1], True)
    all_ref[...] = jnp.sum(s2[...], axis=0)

    settle(rbuf.at[pl.ds(1, nmem - 1)], p1_sem.at[0], False)
    pl.when(sy < nsy - 1)(lambda: settle(pack, e_send.at[0], False))
    pl.when(sy > 0)(lambda: settle(pack, e_send.at[1], False))
    settle(hsend.at[pl.ds(0, nmem - 1)], h_sem.at[0], False)
    settle(s1.at[pl.ds(1, ring - 1)], s1_sem.at[0], False)
    settle(mmsg.at[pl.ds(0, nmem - 1)], m_sem.at[0], False)
    settle(msg.at[pl.ds(0, nmem - 1)], q_sem.at[0], False)
    pl.when(sends_down | sends_up)(lambda: settle(q.at[pl.ds(0, levels)], n_send.at[0], False))
    settle(s2.at[pl.ds(1, len(others))], s2_sem.at[0], False)


def scale(count, z_ref, all_ref, means_ref, mean_ref, cov_ref):
    levels, rows, cols = cov_ref.shape
    spread = jnp.sum(all_ref[...], keepdims=True) * (1.0 / count)
    inverse = 1.0 / (spread + 1e-6)
    for k in range(levels):
        for c in range(cols // LANES):
            block = z_ref[c, pl.ds(k * rows, rows), :]
            cov_ref[k, :, pl.ds(c * LANES, LANES)] = block * inverse
    for i in range(rows):
        inner = 1 if REACH <= i < rows - REACH else 0
        source = i - REACH if inner else i % (rows - 2 * REACH)
        for c in range(cols // LANES):
            row = means_ref[source, pl.ds(2 * inner + c, 1), :]
            mean_ref[0, pl.ds(i, 1), pl.ds(c * LANES, LANES)] = row


def solution(mesh):
    nmem, nsx, nsy = (mesh.shape[name] for name in ("mem", "sx", "sy"))

    def local(child):
        members, levels, child_rows, child_cols = child.shape
        rows, cols = child_rows // 3, child_cols // 3
        f32 = jnp.float32
        dma = pltpu.SemaphoreType.DMA
        vmem = pl.BlockSpec(memory_space=pltpu.VMEM)
        vector = (SUB, LANES)
        z, total, means = pl.pallas_call(
            functools.partial(gather, nmem, nsx, nsy),
            out_shape=(
                jax.ShapeDtypeStruct((2, levels * rows, LANES), f32),
                jax.ShapeDtypeStruct((1, LANES), f32),
                jax.ShapeDtypeStruct((nmem, *vector), f32),
            ),
            in_specs=[pl.BlockSpec(memory_space=pltpu.MemorySpace.HBM)],
            out_specs=(vmem, vmem, vmem),
            scratch_shapes=[
                pltpu.VMEM((2, members, levels, child_rows // 2, child_cols), child.dtype),
                pltpu.VMEM((3 * LANES, LANES), child.dtype),
                pltpu.VMEM((2, members * levels * child_rows // 2, LANES), f32),
                pltpu.VMEM((2, nmem // 2, 16, *vector), f32),
                pltpu.VMEM((nmem, 16, *vector), f32),
                pltpu.VMEM((nmem, *vector), f32),
                pltpu.VMEM((nmem, *vector), f32),
                pltpu.VMEM((nmem, *vector), f32),
                pltpu.VMEM((nmem, *vector), f32),
                pltpu.VMEM((nmem, *vector), f32),
                pltpu.VMEM((4, nmem, *vector), f32),
                pltpu.VMEM((nmem * members, *vector), f32),
                pltpu.VMEM((4, *vector), f32),
                pltpu.VMEM((levels, *vector), f32),
                pltpu.VMEM((nmem, *vector), f32),
                pltpu.VMEM((levels, 5, *vector), f32),
                pltpu.VMEM((rows + 2 * REACH, 3, *vector), f32),
                pltpu.VMEM((nmem, *vector), f32),
                pltpu.VMEM((nmem // 2, 1, LANES), f32),
                pltpu.VMEM((2 * nsx * nsy, 1, LANES), f32),
                dma((2,)),
                dma((4,)),
                dma((2,)),
                dma((2,)),
                dma((2,)),
                dma((2,)),
                dma((2,)),
                dma((2,)),
                dma((1,)),
                dma((2,)),
                dma((2,)),
                pltpu.SemaphoreType.REGULAR((2,)),
            ],
            compiler_params=pltpu.CompilerParams(collective_id=0, has_side_effects=True, vmem_limit_bytes=VMEM_GRANT),
            name="gather",
        )(child)
        count = 4.0 * 81.0 * (members * nmem - 1) * levels * rows * nsx * cols * nsy
        return pl.pallas_call(
            functools.partial(scale, count),
            out_shape=(
                jax.ShapeDtypeStruct((levels // nmem, rows, cols), f32),
                jax.ShapeDtypeStruct((levels, rows, cols), f32),
            ),
            in_specs=[vmem, vmem, vmem],
            out_specs=(vmem, vmem),
            compiler_params=pltpu.CompilerParams(vmem_limit_bytes=8 << 20),
            name="scale",
        )(z, total, means)

    return jax.shard_map(
        local,
        mesh=mesh,
        in_specs=(P("mem", None, "sx", "sy"),),
        out_specs=(P("mem", "sx", "sy"), P("mem", "sx", "sy")),
        check_vma=False,
    )
```
